128 devices in a mesh: replica: 16 (over x, z), tensor: 8 (over y, core).
Axes of the slice: x: 4, y: 4, z: 4, core: 2. Of those that a mesh axis runs over, the one named last changes fastest.
Arguments:
- queries: bfloat16 [1024, 8192], P('replica', 'tensor'), may hold values from -18 to 18
- kv_new: bfloat16 [1024, 2, 1024], P('replica', None, 'tensor'), may hold values from -7.5 to 7.5
- pool: bfloat16 [768, 128, 2, 1024], P('replica', None, None, 'tensor'), may hold values from -240 to 240
- page_table: int32 [32, 12], P('replica'), may hold values from 0 to 767, as said below
- hist_len: int32 [32], P('replica'), may hold values from 769 to 1536
- o_weight: bfloat16 [8192, 8192], P('tensor'), may hold values from -0.125 to 0.125
Outputs:
- mixed: bfloat16 [1024, 8192], P(('replica', 'tensor'))
The draws below stay inside these ranges and needn't reach their ends.
Inputs may be any that keep to these rules, and one draw needn't show every extreme that they name: `page_table`: no two entries are equal. The owner of page id g is the replica group g // 48. Among the live pages (entry j of conversation c with j * 128 < hist_len[c]) of the conversations of one replica group, at most 3 have any one owner, and in every group some owner holds exactly 3 of them.
All inputs are finite; a program needn't handle non-finite values.
Results may differ from the reference program's by a relative error of at most 0.014.
Values may be sent and summed in bfloat16 or wider, within the bound.
No kernel may reach another device: no remote copies, remote signals or barrier semaphores. Data moves between devices by JAX's collectives and lax.ppermute only.
A program may use at most 128 MiB of HBM per device.

```python
import math
import jax
import jax.numpy as jnp
from jax import lax

HEADS = 64
KV_HEADS = 8
HD = 128
D = 8192
NEW = 32
CONV_DEV = 2
PAGE = 128
MAXP = 12
SLOT = 3
CONVS = 32
TOKENS = 1024
POOL_DEV = 48
POOL_PAGES = 768
N_TENSOR = 8


def draw_pool(key, part):
    base = jax.random.truncated_normal(key, -6.0, 6.0, (POOL_PAGES, PAGE, 2, KV_HEADS * HD), jnp.float32)
    return base.astype(jnp.bfloat16)


def draw_page_table(key, part):
    groups = CONVS // CONV_DEV
    width = groups * SLOT
    shelves = jax.vmap(lambda owner: jax.random.permutation(jax.random.fold_in(key, 5000 + owner), POOL_DEV))(jnp.arange(groups, dtype=jnp.int32))

    def one_group(group):
        sub = jax.random.fold_in(key, group)
        first = jax.random.randint(jax.random.fold_in(sub, 1), (), 0, groups)
        shuffled = jax.random.permutation(jax.random.fold_in(sub, 2), width).astype(jnp.int32)
        owner_of = jnp.arange(width, dtype=jnp.int32) // SLOT
        score = shuffled - width * (owner_of == first).astype(jnp.int32)
        chosen = jnp.argsort(score, stable=True)[:CONV_DEV * MAXP].astype(jnp.int32)
        owners = chosen // SLOT
        within = chosen % SLOT
        shelf = shelves[owners, group * SLOT + within]
        table = (owners * POOL_DEV + shelf).reshape(CONV_DEV, MAXP)
        front = jax.random.permutation(jax.random.fold_in(sub, 3), MAXP // 2)
        table = table.at[:, :MAXP // 2].set(table[:, front])
        turn = jax.random.randint(jax.random.fold_in(sub, 4), (), 0, CONV_DEV)
        return jnp.roll(table, turn, axis=0)
    return jax.vmap(one_group)(jnp.arange(groups, dtype=jnp.int32)).reshape(CONVS, MAXP).astype(jnp.int32)


def set_ends(entries, own_key, smallest, high):
    extent = entries.shape
    index_at = [jax.random.randint(jax.random.fold_in(own_key, axis), (), 0, extent[axis]) for axis in range(len(extent))]
    entries = entries.at[tuple(index_at)].set(smallest)
    longest = extent.index(max(extent))
    index_at[longest] = (index_at[longest] + 1) % extent[longest]
    return entries.at[tuple(index_at)].set(high)


def level_of(stream_key, dims, pieces, least, top_value):
    def one(position, shards_of):
        heights = jax.random.uniform(jax.random.fold_in(jax.random.fold_in(stream_key, 6), position), (shards_of,), jnp.float32, least / len(pieces), top_value / len(pieces))
        return jnp.repeat(jnp.exp(heights), dims[position] // shards_of).reshape((-1,) + (1,) * (len(dims) - position - 1))

    gain = one(*pieces[0])
    for cut in pieces[1:]:
        gain = gain * one(*cut)
    return gain


def normal_values(stream_key, shape, spread, limit, shards=(), kind=jnp.bfloat16):
    loudness = level_of(stream_key, shape, shards, -0.22, 0.18) if shards else 1.0
    values = jax.random.normal(stream_key, shape, jnp.float32) * spread * loudness
    return jnp.minimum(jnp.maximum(values, -limit), limit).astype(kind)


def setup_inputs(seed: int = 0) -> dict:
    arg_keys = jax.random.split(jax.random.key(seed), 7)
    return {
        "queries": normal_values(arg_keys[0], (TOKENS, HEADS * HD), 3.0, 18.0, ((0, 16), (1, 8))),
        "kv_new": normal_values(arg_keys[1], (TOKENS, 2, KV_HEADS * HD), 1.25, 7.5, ((0, 16), (2, 8))),
        "pool": draw_pool(jax.random.fold_in(arg_keys[6], 71), 0),
        "page_table": draw_page_table(jax.random.fold_in(arg_keys[6], 71), 0),
        "hist_len": set_ends(jax.random.randint(arg_keys[4], (CONVS,), MAXP * PAGE // 2 + 1, MAXP * PAGE + 1), jax.random.fold_in(arg_keys[4], 1), MAXP * PAGE // 2 + 1, MAXP * PAGE).astype(jnp.int32),
        "o_weight": normal_values(arg_keys[5], (HEADS * HD, D), (HEADS * HD // 4) ** -0.5, 0.125, ((0, 8),)),
    }


floor_value = -1e+30

def attend_part(asked, keys, values, allowed):
    scores = jnp.einsum('nkgd,tkd->nkgt', asked.astype(jnp.float32), keys.astype(jnp.float32)) / math.sqrt(HD)
    peak = lax.optimization_barrier(jnp.max(jnp.where(allowed, scores, floor_value), axis=-1))
    weights = jnp.where(allowed, jnp.exp(scores - peak[..., None]), 0.0).astype(jnp.bfloat16)
    weights = lax.optimization_barrier(weights).astype(jnp.float32)
    amount = lax.optimization_barrier(jnp.sum(weights, axis=-1))
    summed = jnp.einsum('nkgt,tkd->nkgd', weights, values.astype(jnp.float32))
    return (peak, amount, summed)

def merge(first, second):
    peak = jnp.maximum(first[0], second[0])
    keep = jnp.exp(first[0] - peak)
    take = jnp.exp(second[0] - peak)
    return (peak, keep * first[1] + take * second[1], keep[..., None] * first[2] + take[..., None] * second[2])

def reference(queries, kv_new, pool, page_table, hist_len, o_weight):
    per_group = HEADS // KV_HEADS
    asked_all = queries.reshape(CONVS, NEW, KV_HEADS, per_group, HD)
    fresh_all = kv_new.reshape(CONVS, NEW, 2, KV_HEADS, HD)
    pool_all = pool.reshape(POOL_PAGES, PAGE, 2, KV_HEADS, HD)
    order = jnp.arange(NEW, dtype=jnp.int32)
    causal = (order[None, :] <= order[:, None])[:, None, None, :]
    inside = jnp.arange(PAGE, dtype=jnp.int32)

    def one_dialog(items):
        asked, fresh, table, length = items
        state = attend_part(asked, fresh[:, 0], fresh[:, 1], causal)

        def step(carry, index):
            page = pool_all[table[index]]
            live = index * PAGE + inside < length
            part = attend_part(asked, page[:, 0], page[:, 1], live[None, None, None, :])
            used = index * PAGE < length
            merged = merge(carry, part)
            return (jax.tree.map(lambda fresh_value, old_value: jnp.where(used, fresh_value, old_value), merged, carry), None)
        state, _ = lax.scan(step, state, jnp.arange(MAXP, dtype=jnp.int32))
        attended = (state[2] / state[1][..., None]).astype(jnp.bfloat16)
        return attended.reshape(NEW, HEADS * HD)
    attended = lax.map(one_dialog, (asked_all, fresh_all, page_table, hist_len)).reshape(TOKENS, N_TENSOR, HEADS * HD // N_TENSOR)
    blocks = o_weight.reshape(N_TENSOR, HEADS * HD // N_TENSOR, D)

    def add_block(running, index):
        part = jnp.dot(attended[:, index], blocks[index], preferred_element_type=jnp.float32)
        part = lax.optimization_barrier(part.astype(jnp.bfloat16)).astype(jnp.float32)
        return (running + part, None)
    running, _ = lax.scan(add_block, jnp.zeros((TOKENS, D), jnp.float32), jnp.arange(N_TENSOR, dtype=jnp.int32))
    return running.astype(jnp.bfloat16)
```

```python
import functools
import math

import jax
import jax.numpy as jnp
from jax import lax
from jax.experimental import pallas as pl
from jax.experimental.pallas import tpu as pltpu
from jax.sharding import Mesh
from jax.sharding import PartitionSpec as P

HD = 128
PAGE = 128
SLOT = 3
LANES = 128
FLOOR = -1e30
REPLICA = ("replica_0", "replica_1")
TENSOR = ("row", "core")


def plan_kernel(groups, pool_size, table, length, wanted, place, count):
    dialogs, entries = table.shape

    def clear(owner, _):
        count[owner] = 0
        for slot in range(SLOT):
            wanted[owner, 0, slot] = 0
        return 0

    lax.fori_loop(0, groups, clear, 0)

    def one(index, _):
        dialog = index // entries
        entry = index % entries
        page = table[dialog, entry]
        owner = page // pool_size
        live = entry * PAGE < length[dialog]
        rank = count[owner]

        @pl.when(live)
        def _():
            wanted[owner, 0, rank] = page - owner * pool_size
            count[owner] = rank + 1

        place[dialog, entry] = jnp.where(live, owner * SLOT + rank, 0)
        return 0

    lax.fori_loop(0, dialogs * entries, one, 0)


def plan(page_table, hist_len, groups, pool_size):
    smem = pl.BlockSpec(memory_space=pltpu.SMEM)
    return pl.pallas_call(
        functools.partial(plan_kernel, groups, pool_size),
        out_shape=(
            jax.ShapeDtypeStruct((groups, 1, LANES), jnp.int32),
            jax.ShapeDtypeStruct(page_table.shape, jnp.int32),
        ),
        in_specs=[smem, smem],
        out_specs=(smem, smem),
        scratch_shapes=[pltpu.SMEM((groups,), jnp.int32)],
        name="plan",
    )(page_table, hist_len)


def collect_kernel(groups, asked, pool, out, held, came, left):
    def arrive(owner, slot):
        return pltpu.make_async_copy(
            pool.at[asked[owner, 0, slot]], held.at[owner, slot], came.at[owner, slot]
        )

    def leave(owner):
        return pltpu.make_async_copy(held.at[owner], out.at[owner], left.at[owner])

    for owner in range(groups):
        for slot in range(SLOT):
            arrive(owner, slot).start()
    for owner in range(groups):
        for slot in range(SLOT):
            arrive(owner, slot).wait()
        leave(owner).start()
    for owner in range(groups):
        leave(owner).wait()


def collect(asked, pool, groups):
    shape = (groups, SLOT) + pool.shape[1:]
    return pl.pallas_call(
        functools.partial(collect_kernel, groups),
        out_shape=jax.ShapeDtypeStruct(shape, pool.dtype),
        in_specs=[
            pl.BlockSpec(memory_space=pltpu.SMEM),
            pl.BlockSpec(memory_space=pl.ANY),
        ],
        out_specs=pl.BlockSpec(memory_space=pl.ANY),
        scratch_shapes=[
            pltpu.VMEM(shape, pool.dtype),
            pltpu.SemaphoreType.DMA((groups, SLOT)),
            pltpu.SemaphoreType.DMA((groups,)),
        ],
        name="collect",
    )(asked, pool)


def attend_kernel(
    tensor_rows,
    place,
    length,
    core,
    queries,
    keys_new,
    values_new,
    pages,
    weight,
    give,
    keep,
    held,
    panel,
    mixed,
    page_sem,
    panel_sem,
):
    dialogs, entries = place.shape
    rows = queries.shape[0]
    fresh = rows // dialogs
    heads = queries.shape[1] // HD
    panels = panel.shape[0]
    width = panel.shape[2]

    def page_copy(dialog, entry):
        return pltpu.make_async_copy(
            pages.at[place[dialog, entry]], held.at[dialog, entry], page_sem.at[dialog, entry]
        )

    def panel_copy(index):
        return pltpu.make_async_copy(
            weight.at[:, pl.ds(index * width, width)], panel.at[index], panel_sem.at[index]
        )

    for dialog in range(dialogs):
        for entry in range(entries):
            page_copy(dialog, entry).start()
    for index in range(panels):
        panel_copy(index).start()

    scale = 1.0 / math.sqrt(HD)
    nt = (((1,), (1,)), ((), ()))
    nn = (((1,), (0,)), ((), ()))
    pieces = []
    for dialog in range(dialogs):
        own = slice(dialog * fresh, (dialog + 1) * fresh)
        asked = jnp.concatenate(
            [queries[own, head * HD : (head + 1) * HD] for head in range(heads)], axis=0
        )
        score_new = (
            lax.dot_general(asked, keys_new[own, :], nt, preferred_element_type=jnp.float32) * scale
        )
        row = lax.broadcasted_iota(jnp.int32, score_new.shape, 0) % fresh
        col = lax.broadcasted_iota(jnp.int32, score_new.shape, 1)
        score_new = jnp.where(col <= row, score_new, FLOOR)
        for entry in range(entries):
            page_copy(dialog, entry).wait()
        keys = held[dialog, :, 0].reshape(entries * PAGE, HD)
        values = held[dialog, :, 1].reshape(entries * PAGE, HD)
        score = lax.dot_general(asked, keys, nt, preferred_element_type=jnp.float32) * scale
        token = lax.broadcasted_iota(jnp.int32, score.shape, 1)
        score = jnp.where(token < length[dialog], score, FLOOR)
        peak = jnp.maximum(
            jnp.max(score, axis=1, keepdims=True), jnp.max(score_new, axis=1, keepdims=True)
        )
        part = jnp.exp(score - peak).astype(jnp.bfloat16)
        part_new = jnp.exp(score_new - peak).astype(jnp.bfloat16)
        amount = jnp.sum(part.astype(jnp.float32), axis=1, keepdims=True) + jnp.sum(
            part_new.astype(jnp.float32), axis=1, keepdims=True
        )
        summed = lax.dot_general(
            part, values, nn, preferred_element_type=jnp.float32
        ) + lax.dot_general(part_new, values_new[own, :], nn, preferred_element_type=jnp.float32)
        attended = summed / amount
        pieces.append(
            jnp.concatenate(
                [attended[head * fresh : (head + 1) * fresh, :] for head in range(heads)], axis=1
            )
        )
    attended = jnp.concatenate(pieces, axis=0)
    block = rows // (2 * tensor_rows)
    sides = [
        jnp.concatenate(
            [
                attended[(2 * index + side) * block : (2 * index + side + 1) * block, :]
                for index in range(tensor_rows)
            ],
            axis=0,
        )
        for side in range(2)
    ]
    first = core[0] == 0
    mixed[...] = jnp.concatenate(
        [jnp.where(first, sides[1], sides[0]), jnp.where(first, sides[0], sides[1])], axis=0
    ).astype(jnp.bfloat16)
    half = rows // 2
    for index in range(panels):
        panel_copy(index).wait()
        product = lax.dot_general(
            mixed[...], panel[index], nn, preferred_element_type=jnp.float32
        ).astype(jnp.bfloat16)
        give[:, index * width : (index + 1) * width] = product[:half]
        keep[:, index * width : (index + 1) * width] = product[half:]


def attend(place, hist_len, core, queries, keys_new, values_new, pages, weight, tensor_rows):
    dialogs, entries = place.shape
    rows = queries.shape[0]
    panels = 8
    out = jax.ShapeDtypeStruct((rows // 2, weight.shape[1]), jnp.bfloat16)
    smem = pl.BlockSpec(memory_space=pltpu.SMEM)
    vmem = pl.BlockSpec(memory_space=pltpu.VMEM)
    hbm = pl.BlockSpec(memory_space=pl.ANY)
    return pl.pallas_call(
        functools.partial(attend_kernel, tensor_rows),
        out_shape=(out, out),
        in_specs=[smem, smem, smem, vmem, vmem, vmem, hbm, hbm],
        out_specs=(vmem, vmem),
        scratch_shapes=[
            pltpu.VMEM((dialogs, entries) + pages.shape[1:], pages.dtype),
            pltpu.VMEM((panels, weight.shape[0], weight.shape[1] // panels), weight.dtype),
            pltpu.VMEM((rows, weight.shape[0]), jnp.bfloat16),
            pltpu.SemaphoreType.DMA((dialogs, entries)),
            pltpu.SemaphoreType.DMA((panels,)),
        ],
        compiler_params=pltpu.CompilerParams(vmem_limit_bytes=48 * 1024 * 1024),
        name="attend",
    )(place, hist_len, core, queries, keys_new, values_new, pages, weight)


def local(queries, kv_new, pool, page_table, hist_len, o_weight):
    groups = lax.axis_size(REPLICA)
    pool_size = pool.shape[0]
    tensor_rows = lax.axis_size("row")
    wanted, place = plan(page_table, hist_len, groups, pool_size)
    asked = lax.all_to_all(wanted, REPLICA, split_axis=0, concat_axis=0, tiled=True)
    shelves = jnp.swapaxes(pool, 1, 2)
    sent = collect(asked, shelves, groups)
    pages = lax.all_to_all(sent, REPLICA, split_axis=0, concat_axis=0, tiled=True)
    pages = pages.reshape((groups * SLOT,) + pages.shape[2:])
    core = lax.axis_index("core").astype(jnp.int32).reshape(1)
    give, keep = attend(
        place, hist_len, core, queries, kv_new[:, 0], kv_new[:, 1], pages, o_weight, tensor_rows
    )
    came = lax.ppermute(give, "core", [(0, 1), (1, 0)])
    pair = (keep.astype(jnp.float32) + came.astype(jnp.float32)).astype(jnp.bfloat16)
    pair = pair.reshape(tensor_rows, -1, pair.shape[1])
    blocks = lax.all_to_all(pair, "row", split_axis=0, concat_axis=0, tiled=True)
    return jnp.sum(blocks.astype(jnp.float32), axis=0).astype(jnp.bfloat16)


def solution(mesh):
    split = Mesh(
        mesh.devices.reshape(4, 4, mesh.shape["tensor"] // 2, 2), REPLICA + TENSOR
    )
    in_specs = (
        P(REPLICA, TENSOR),
        P(REPLICA, None, TENSOR),
        P(REPLICA, None, None, TENSOR),
        P(REPLICA, None),
        P(REPLICA),
        P(TENSOR, None),
    )
    out_specs = P(REPLICA + TENSOR, None)
    return jax.shard_map(local, mesh=split, in_specs=in_specs, out_specs=out_specs, check_vma=False)
```

```python
import functools
import math

import jax
import jax.numpy as jnp
from jax import lax
from jax.experimental import pallas as pl
from jax.experimental.pallas import tpu as pltpu
from jax.sharding import Mesh
from jax.sharding import PartitionSpec as P

HD = 128
PAGE = 128
SLOT = 3
LANES = 128
FLOOR = -1e30
REPLICA = ("replica_0", "replica_1")
TENSOR = ("row", "core")


def plan_kernel(groups, table, length, pool, wanted, place, near, count, near_sem):
    bring = pltpu.make_async_copy(pool, near, near_sem)
    bring.start()
    dialogs, entries = table.shape
    pool_size = pool.shape[0]
    for owner in range(groups):
        count[owner] = 0
        for slot in range(SLOT):
            wanted[owner, 0, slot] = 0
    for dialog in range(dialogs):
        tokens = length[dialog]
        for entry in range(entries):
            page = table[dialog, entry]
            owner = lax.div(page, pool_size)
            live = entry * PAGE < tokens
            rank = count[owner]

            @pl.when(live)
            def _():
                wanted[owner, 0, rank] = page - owner * pool_size
                count[owner] = rank + 1

            place[dialog, entry] = jnp.where(live, owner * SLOT + rank, 0)
    bring.wait()


def plan(page_table, hist_len, pool, groups):
    smem = pl.BlockSpec(memory_space=pltpu.SMEM)
    return pl.pallas_call(
        functools.partial(plan_kernel, groups),
        out_shape=(
            jax.ShapeDtypeStruct((groups, 1, LANES), jnp.int32),
            jax.ShapeDtypeStruct(page_table.shape, jnp.int32),
            jax.ShapeDtypeStruct(pool.shape, pool.dtype),
        ),
        in_specs=[smem, smem, pl.BlockSpec(memory_space=pltpu.HBM)],
        out_specs=(smem, smem, pl.BlockSpec(memory_space=pltpu.VMEM)),
        scratch_shapes=[pltpu.SMEM((groups,), jnp.int32), pltpu.SemaphoreType.DMA],
        compiler_params=pltpu.CompilerParams(vmem_limit_bytes=50 * 1024 * 1024),
        name="plan",
    )(page_table, hist_len, pool)


def collect_kernel(groups, asked, pool, out, ids, ids_sem):
    read = pltpu.make_async_copy(asked, ids, ids_sem)
    read.start()
    read.wait()
    for owner in range(groups):
        for slot in range(SLOT):
            out[owner, slot] = pool[ids[owner, 0, slot]]


def collect(asked, pool, groups):
    shape = (groups, SLOT) + pool.shape[1:]
    vmem = pl.BlockSpec(memory_space=pltpu.VMEM)
    return pl.pallas_call(
        functools.partial(collect_kernel, groups),
        out_shape=jax.ShapeDtypeStruct(shape, pool.dtype),
        in_specs=[pl.BlockSpec(memory_space=pl.ANY), vmem],
        out_specs=vmem,
        scratch_shapes=[pltpu.SMEM(asked.shape, jnp.int32), pltpu.SemaphoreType.DMA],
        compiler_params=pltpu.CompilerParams(vmem_limit_bytes=8 * 1024 * 1024),
        name="collect",
    )(asked, pool)


def attend_kernel(
    tensor_rows,
    place,
    length,
    queries,
    kv_new,
    pages,
    weight,
    give,
    keep,
    wide,
    wide_new,
    keys,
    values,
    mixed,
    panel,
    panel_sem,
):
    dialogs, entries = place.shape
    rows = queries.shape[0]
    fresh = rows // dialogs
    heads = queries.shape[1] // HD
    panels = panel.shape[0]
    width = panel.shape[2]

    def panel_copy(index):
        return pltpu.make_async_copy(
            weight.at[:, pl.ds(index * width, width)], panel.at[index], panel_sem.at[index]
        )

    for index in range(panels):
        panel_copy(index).start()

    scale = 1.0 / math.sqrt(HD)
    nt = (((1,), (1,)), ((), ()))
    nn = (((1,), (0,)), ((), ()))
    wide_new[...] = kv_new[...].astype(jnp.float32)
    for dialog in range(dialogs):
        for entry in range(entries):
            wide[dialog, entry] = pages[place[dialog, entry]].astype(jnp.float32)
            span = slice(entry * PAGE, (entry + 1) * PAGE)
            keys[dialog, span, :] = wide[dialog, entry, pl.ds(0, PAGE, stride=2), :].astype(
                jnp.bfloat16
            )
            values[dialog, span, :] = wide[dialog, entry, pl.ds(1, PAGE, stride=2), :].astype(
                jnp.bfloat16
            )
    pieces = []
    for dialog in range(dialogs):
        own = slice(dialog * fresh, (dialog + 1) * fresh)
        asked = jnp.concatenate(
            [queries[own, head * HD : (head + 1) * HD] for head in range(heads)], axis=0
        )
        start = dialog * 2 * fresh
        keys_new = wide_new[pl.ds(start, fresh, stride=2), :].astype(jnp.bfloat16)
        values_new = wide_new[pl.ds(start + 1, fresh, stride=2), :].astype(jnp.bfloat16)
        score_new = (
            lax.dot_general(asked, keys_new, nt, preferred_element_type=jnp.float32) * scale
        )
        row = lax.broadcasted_iota(jnp.int32, score_new.shape, 0) % fresh
        col = lax.broadcasted_iota(jnp.int32, score_new.shape, 1)
        score_new = jnp.where(col <= row, score_new, FLOOR)
        score = lax.dot_general(asked, keys[dialog], nt, preferred_element_type=jnp.float32) * scale
        token = lax.broadcasted_iota(jnp.int32, score.shape, 1)
        score = jnp.where(token < length[dialog], score, FLOOR)
        peak = jnp.maximum(
            jnp.max(score, axis=1, keepdims=True), jnp.max(score_new, axis=1, keepdims=True)
        )
        part = jnp.exp(score - peak).astype(jnp.bfloat16)
        part_new = jnp.exp(score_new - peak).astype(jnp.bfloat16)
        amount = jnp.sum(part.astype(jnp.float32), axis=1, keepdims=True) + jnp.sum(
            part_new.astype(jnp.float32), axis=1, keepdims=True
        )
        summed = lax.dot_general(
            part, values[dialog], nn, preferred_element_type=jnp.float32
        ) + lax.dot_general(part_new, values_new, nn, preferred_element_type=jnp.float32)
        attended = summed / amount
        pieces.append(
            jnp.concatenate(
                [attended[head * fresh : (head + 1) * fresh, :] for head in range(heads)], axis=1
            )
        )
    attended = jnp.concatenate(pieces, axis=0)
    block = rows // (2 * tensor_rows)
    sides = [
        jnp.concatenate(
            [
                attended[(2 * index + side) * block : (2 * index + side + 1) * block, :]
                for index in range(tensor_rows)
            ],
            axis=0,
        )
        for side in range(2)
    ]
    first = lax.axis_index("core") == 0
    mixed[...] = jnp.concatenate(
        [jnp.where(first, sides[1], sides[0]), jnp.where(first, sides[0], sides[1])], axis=0
    ).astype(jnp.bfloat16)
    half = rows // 2
    for index in range(panels):
        span = slice(index * width, (index + 1) * width)
        panel_copy(index).wait()
        product = lax.dot_general(
            mixed[...], panel[index], nn, preferred_element_type=jnp.float32
        ).astype(jnp.bfloat16)
        give[:, span] = product[:half]
        keep[:, span] = product[half:]


def attend(place, hist_len, queries, kv_new, pages, weight, tensor_rows):
    dialogs, entries = place.shape
    rows = queries.shape[0]
    out = jax.ShapeDtypeStruct((rows // 2, weight.shape[1]), jnp.bfloat16)
    smem = pl.BlockSpec(memory_space=pltpu.SMEM)
    vmem = pl.BlockSpec(memory_space=pltpu.VMEM)
    panels = 8
    history = (dialogs, entries * PAGE, HD)
    return pl.pallas_call(
        functools.partial(attend_kernel, tensor_rows),
        out_shape=(out, out),
        in_specs=[smem, smem, vmem, vmem, vmem, pl.BlockSpec(memory_space=pltpu.HBM)],
        out_specs=(vmem, vmem),
        scratch_shapes=[
            pltpu.VMEM((dialogs, entries) + pages.shape[1:], jnp.float32),
            pltpu.VMEM(kv_new.shape, jnp.float32),
            pltpu.VMEM(history, jnp.bfloat16),
            pltpu.VMEM(history, jnp.bfloat16),
            pltpu.VMEM((rows, weight.shape[0]), jnp.bfloat16),
            pltpu.VMEM((panels, weight.shape[0], weight.shape[1] // panels), weight.dtype),
            pltpu.SemaphoreType.DMA((panels,)),
        ],
        compiler_params=pltpu.CompilerParams(vmem_limit_bytes=48 * 1024 * 1024),
        name="attend",
    )(place, hist_len, queries, kv_new, pages, weight)


def local(queries, kv_new, pool, page_table, hist_len, o_weight):
    groups = lax.axis_size(REPLICA)
    tensor_rows = lax.axis_size("row")
    shelves = pool.reshape(pool.shape[0], 2 * PAGE, HD)
    wanted, place, shelves = plan(page_table, hist_len, shelves, groups)
    asked = lax.all_to_all(wanted, REPLICA, split_axis=0, concat_axis=0, tiled=True)
    sent = collect(asked, shelves, groups)
    pages = lax.all_to_all(sent, REPLICA, split_axis=0, concat_axis=0, tiled=True)
    pages = pages.reshape(groups * SLOT, 2 * PAGE, HD)
    fresh = kv_new.reshape(2 * kv_new.shape[0], HD)
    give, keep = attend(place, hist_len, queries, fresh, pages, o_weight, tensor_rows)
    came = lax.ppermute(give, "core", [(0, 1), (1, 0)])
    pair = (keep.astype(jnp.float32) + came.astype(jnp.float32)).astype(jnp.bfloat16)
    pair = pair.reshape(tensor_rows, -1, pair.shape[1])
    blocks = lax.all_to_all(pair, "row", split_axis=0, concat_axis=0, tiled=True)
    return jnp.sum(blocks.astype(jnp.float32), axis=0).astype(jnp.bfloat16)


def solution(mesh):
    split = Mesh(
        mesh.devices.reshape(4, 4, mesh.shape["tensor"] // 2, 2), REPLICA + TENSOR
    )
    in_specs = (
        P(REPLICA, TENSOR),
        P(REPLICA, None, TENSOR),
        P(REPLICA, None, None, TENSOR),
        P(REPLICA, None),
        P(REPLICA),
        P(TENSOR, None),
    )
    out_specs = P(REPLICA + TENSOR, None)
    return jax.shard_map(local, mesh=split, in_specs=in_specs, out_specs=out_specs, check_vma=False)
```

```python
import functools
import math

import jax
import jax.numpy as jnp
from jax import lax
from jax.experimental import pallas as pl
from jax.experimental.pallas import tpu as pltpu
from jax.sharding import Mesh
from jax.sharding import PartitionSpec as P

HD = 128
PAGE = 128
SLOT = 3
LANES = 128
PANELS = 8
FLOOR = -1e30
REPLICA = ("replica_0", "replica_1")
TENSOR = ("row", "core")


def plan_kernel(groups, table, length, pool, wanted, place, near, count, near_sem):
    bring = pltpu.make_async_copy(pool, near, near_sem)
    bring.start()
    dialogs, entries = table.shape
    pool_size = pool.shape[0]
    for owner in range(groups):
        count[owner] = 0
        for slot in range(SLOT):
            wanted[owner, 0, slot] = 0
    for dialog in range(dialogs):
        tokens = length[dialog]
        for entry in range(entries):
            page = table[dialog, entry]
            owner = lax.div(page, pool_size)
            live = entry * PAGE < tokens
            rank = count[owner]

            @pl.when(live)
            def _():
                wanted[owner, 0, rank] = page - owner * pool_size
                count[owner] = rank + 1

            place[dialog, entry] = jnp.where(live, owner * SLOT + rank, 0)
    bring.wait()


def plan(page_table, hist_len, pool, groups):
    smem = pl.BlockSpec(memory_space=pltpu.SMEM)
    return pl.pallas_call(
        functools.partial(plan_kernel, groups),
        out_shape=(
            jax.ShapeDtypeStruct((groups, 1, LANES), jnp.int32),
            jax.ShapeDtypeStruct(page_table.shape, jnp.int32),
            jax.ShapeDtypeStruct(pool.shape, pool.dtype),
        ),
        in_specs=[smem, smem, pl.BlockSpec(memory_space=pltpu.HBM)],
        out_specs=(smem, smem, pl.BlockSpec(memory_space=pltpu.VMEM)),
        scratch_shapes=[pltpu.SMEM((groups,), jnp.int32), pltpu.SemaphoreType.DMA],
        compiler_params=pltpu.CompilerParams(vmem_limit_bytes=50 * 1024 * 1024),
        name="plan",
    )(page_table, hist_len, pool)


def collect_kernel(groups, asked, pool, out, ids, ids_sem):
    read = pltpu.make_async_copy(asked, ids, ids_sem)
    read.start()
    read.wait()
    for owner in range(groups):
        for slot in range(SLOT):
            out[owner, slot] = pool[ids[owner, 0, slot]]


def collect(asked, pool, groups):
    shape = (groups, SLOT) + pool.shape[1:]
    vmem = pl.BlockSpec(memory_space=pltpu.VMEM)
    return pl.pallas_call(
        functools.partial(collect_kernel, groups),
        out_shape=jax.ShapeDtypeStruct(shape, pool.dtype),
        in_specs=[pl.BlockSpec(memory_space=pl.ANY), vmem],
        out_specs=vmem,
        scratch_shapes=[pltpu.SMEM(asked.shape, jnp.int32), pltpu.SemaphoreType.DMA],
        compiler_params=pltpu.CompilerParams(vmem_limit_bytes=8 * 1024 * 1024),
        name="collect",
    )(asked, pool)


def attend_kernel(
    tensor_rows,
    place,
    length,
    queries,
    kv_new,
    pages,
    weight,
    give,
    keep,
    wide,
    wide_new,
    keys,
    values,
    blocks,
    panel,
    panel_sem,
):
    dialogs, entries = place.shape
    rows = queries.shape[0]
    fresh = rows // dialogs
    heads = queries.shape[1] // HD
    block = rows // (2 * tensor_rows)
    panels, _, width = panel.shape

    def panel_copy(index):
        return pltpu.make_async_copy(
            weight.at[:, pl.ds(index * width, width)], panel.at[index], panel_sem.at[index]
        )

    for index in range(panels):
        panel_copy(index).start()

    scale = 1.0 / math.sqrt(HD)
    nt = (((1,), (1,)), ((), ()))
    nn = (((1,), (0,)), ((), ()))
    wide_new[...] = kv_new[...].astype(jnp.float32)
    for dialog in range(dialogs):
        for entry in range(entries):
            wide[dialog, entry] = pages[place[dialog, entry]].astype(jnp.float32)
            span = slice(entry * PAGE, (entry + 1) * PAGE)
            keys[dialog, span, :] = wide[dialog, entry, pl.ds(0, PAGE, stride=2), :].astype(
                jnp.bfloat16
            )
            values[dialog, span, :] = wide[dialog, entry, pl.ds(1, PAGE, stride=2), :].astype(
                jnp.bfloat16
            )
    pieces = []
    for dialog in range(dialogs):
        own = slice(dialog * fresh, (dialog + 1) * fresh)
        asked = jnp.concatenate(
            [queries[own, head * HD : (head + 1) * HD] for head in range(heads)], axis=0
        )
        start = dialog * 2 * fresh
        keys_new = wide_new[pl.ds(start, fresh, stride=2), :].astype(jnp.bfloat16)
        values_new = wide_new[pl.ds(start + 1, fresh, stride=2), :].astype(jnp.bfloat16)
        score_new = (
            lax.dot_general(asked, keys_new, nt, preferred_element_type=jnp.float32) * scale
        )
        row = lax.broadcasted_iota(jnp.int32, score_new.shape, 0) % fresh
        col = lax.broadcasted_iota(jnp.int32, score_new.shape, 1)
        score_new = jnp.where(col <= row, score_new, FLOOR)
        score = lax.dot_general(asked, keys[dialog], nt, preferred_element_type=jnp.float32) * scale
        token = lax.broadcasted_iota(jnp.int32, score.shape, 1)
        score = jnp.where(token < length[dialog], score, FLOOR)
        peak = jnp.maximum(
            jnp.max(score, axis=1, keepdims=True), jnp.max(score_new, axis=1, keepdims=True)
        )
        part = jnp.exp(score - peak).astype(jnp.bfloat16)
        part_new = jnp.exp(score_new - peak).astype(jnp.bfloat16)
        amount = jnp.sum(part.astype(jnp.float32), axis=1, keepdims=True) + jnp.sum(
            part_new.astype(jnp.float32), axis=1, keepdims=True
        )
        summed = lax.dot_general(
            part, values[dialog], nn, preferred_element_type=jnp.float32
        ) + lax.dot_general(part_new, values_new, nn, preferred_element_type=jnp.float32)
        attended = summed / amount
        for head in range(heads):
            for index in range(fresh // block):
                first = head * fresh + index * block
                blocks[dialog * (fresh // block) + index, :, head * HD : (head + 1) * HD] = (
                    attended[first : first + block, :]
                )
    row, core = lax.axis_index("row"), lax.axis_index("core")
    across, beside = tensor_rows - 1 - row, row ^ 1
    orders = (
        (row, across, beside, across ^ 1),
        (row, beside, across, across ^ 1),
    )
    half = rows // 2
    sides = weight.shape[1] // len(orders)
    for side, order in enumerate(orders):
        mixed = jnp.concatenate(
            [blocks[2 * there + 1 - core] for there in order]
            + [blocks[2 * there + core] for there in order],
            axis=0,
        ).astype(jnp.bfloat16)
        for index in range(sides // width):
            number = side * (sides // width) + index
            span = slice(index * width, (index + 1) * width)
            panel_copy(number).wait()
            product = lax.dot_general(
                mixed, panel[number], nn, preferred_element_type=jnp.float32
            ).astype(jnp.bfloat16)
            give[side, :, span] = product[:half]
            keep[side, :, span] = product[half:]


def attend(place, hist_len, queries, kv_new, pages, weight, tensor_rows):
    dialogs, entries = place.shape
    rows = queries.shape[0]
    out = jax.ShapeDtypeStruct((2, rows // 2, weight.shape[1] // 2), jnp.bfloat16)
    smem = pl.BlockSpec(memory_space=pltpu.SMEM)
    vmem = pl.BlockSpec(memory_space=pltpu.VMEM)
    hbm = pl.BlockSpec(memory_space=pltpu.HBM)
    history = (dialogs, entries * PAGE, HD)
    return pl.pallas_call(
        functools.partial(attend_kernel, tensor_rows),
        out_shape=(out, out),
        in_specs=[smem, smem, vmem, vmem, vmem, hbm],
        out_specs=(vmem, vmem),
        scratch_shapes=[
            pltpu.VMEM((dialogs, entries) + pages.shape[1:], jnp.float32),
            pltpu.VMEM(kv_new.shape, jnp.float32),
            pltpu.VMEM(history, jnp.bfloat16),
            pltpu.VMEM(history, jnp.bfloat16),
            pltpu.VMEM((2 * tensor_rows, rows // (2 * tensor_rows), weight.shape[0]), jnp.float32),
            pltpu.VMEM((PANELS, weight.shape[0], weight.shape[1] // PANELS), weight.dtype),
            pltpu.SemaphoreType.DMA((PANELS,)),
        ],
        compiler_params=pltpu.CompilerParams(vmem_limit_bytes=48 * 1024 * 1024),
        name="attend",
    )(place, hist_len, queries, kv_new, pages, weight)


def sum_over_tensor(give, keep, tensor_rows):
    swap = [(0, 1), (1, 0)]
    beside = [(row, row ^ 1) for row in range(tensor_rows)]
    across = [(row, tensor_rows - 1 - row) for row in range(tensor_rows)]
    came = lax.ppermute(give, "core", swap)
    half = give.shape[1] // 2
    quarter = half // 2
    wide = jnp.float32
    near = keep[:, :half].astype(wide) + came[:, :half].astype(wide)
    far = (keep[:, half:].astype(wide) + came[:, half:].astype(wide)).astype(give.dtype)
    moved = (
        lax.ppermute(far[0], "row", beside),
        lax.ppermute(far[1], "row", across),
    )
    sums = [near[side] + moved[side].astype(wide) for side in range(2)]
    last = (
        lax.ppermute(sums[0][quarter:].astype(give.dtype), "row", across),
        lax.ppermute(sums[1][quarter:].astype(give.dtype), "row", beside),
    )
    return jnp.concatenate(
        [(sums[side][:quarter] + last[side].astype(wide)).astype(give.dtype) for side in range(2)],
        axis=1,
    )


def local(queries, kv_new, pool, page_table, hist_len, o_weight):
    groups = lax.axis_size(REPLICA)
    tensor_rows = lax.axis_size("row")
    shelves = pool.reshape(pool.shape[0], 2 * PAGE, HD)
    wanted, place, shelves = plan(page_table, hist_len, shelves, groups)
    asked = lax.all_to_all(wanted, REPLICA, split_axis=0, concat_axis=0, tiled=True)
    sent = collect(asked, shelves, groups)
    pages = lax.all_to_all(sent, REPLICA, split_axis=0, concat_axis=0, tiled=True)
    pages = pages.reshape(groups * SLOT, 2 * PAGE, HD)
    fresh = kv_new.reshape(2 * kv_new.shape[0], HD)
    give, keep = attend(place, hist_len, queries, fresh, pages, o_weight, tensor_rows)
    return sum_over_tensor(give, keep, tensor_rows)


def solution(mesh):
    split = Mesh(
        mesh.devices.reshape(4, 4, mesh.shape["tensor"] // 2, 2), REPLICA + TENSOR
    )
    in_specs = (
        P(REPLICA, TENSOR),
        P(REPLICA, None, TENSOR),
        P(REPLICA, None, None, TENSOR),
        P(REPLICA, None),
        P(REPLICA),
        P(TENSOR, None),
    )
    out_specs = P(REPLICA + TENSOR, None)
    return jax.shard_map(local, mesh=split, in_specs=in_specs, out_specs=out_specs, check_vma=False)
```

```python
import functools
import math

import jax
import jax.numpy as jnp
from jax import lax
from jax.experimental import pallas as pl
from jax.experimental.pallas import tpu as pltpu
from jax.sharding import Mesh
from jax.sharding import PartitionSpec as P

HD = 128
PAGE = 128
SLOT = 3
LANES = 128
PANELS = 8
FLOOR = -1e30
REPLICA = ("replica_0", "replica_1")
TENSOR = ("row", "core")


def plan_kernel(groups, pool_size, table, length, wanted, place, count):
    dialogs, entries = table.shape
    for owner in range(groups):
        count[owner] = 0
        for slot in range(SLOT):
            wanted[owner, 0, slot] = 0
    for dialog in range(dialogs):
        tokens = length[dialog]
        for entry in range(entries):
            page = table[dialog, entry]
            owner = lax.div(page, pool_size)
            live = entry * PAGE < tokens
            rank = count[owner]

            @pl.when(live)
            def _():
                wanted[owner, 0, rank] = page - owner * pool_size
                count[owner] = rank + 1

            place[dialog, entry] = jnp.where(live, owner * SLOT + rank, 0)


def plan(page_table, hist_len, groups, pool_size):
    smem = pl.BlockSpec(memory_space=pltpu.SMEM)
    return pl.pallas_call(
        functools.partial(plan_kernel, groups, pool_size),
        out_shape=(
            jax.ShapeDtypeStruct((groups, 1, LANES), jnp.int32),
            jax.ShapeDtypeStruct(page_table.shape, jnp.int32),
        ),
        in_specs=[smem, smem],
        out_specs=(smem, smem),
        scratch_shapes=[pltpu.SMEM((groups,), jnp.int32)],
        compiler_params=pltpu.CompilerParams(vmem_limit_bytes=60000 * 1024),
        cost_estimate=pl.CostEstimate(flops=10**10, bytes_accessed=10**7, transcendentals=0),
        name="plan",
    )(page_table, hist_len)


def collect_kernel(groups, asked, pool, out, ids, ids_sem):
    read = pltpu.make_async_copy(asked, ids, ids_sem)
    read.start()
    read.wait()
    for owner in range(groups):
        for slot in range(SLOT):
            out[owner, slot] = pool[ids[owner, 0, slot]]


def collect(asked, pool, groups):
    shape = (groups, SLOT) + pool.shape[1:]
    vmem = pl.BlockSpec(memory_space=pltpu.VMEM)
    return pl.pallas_call(
        functools.partial(collect_kernel, groups),
        out_shape=jax.ShapeDtypeStruct(shape, pool.dtype),
        in_specs=[pl.BlockSpec(memory_space=pl.ANY), vmem],
        out_specs=vmem,
        scratch_shapes=[pltpu.SMEM(asked.shape, jnp.int32), pltpu.SemaphoreType.DMA],
        compiler_params=pltpu.CompilerParams(vmem_limit_bytes=8 * 1024 * 1024),
        cost_estimate=pl.CostEstimate(flops=100000000000, bytes_accessed=100000000, transcendentals=0),
        name="collect",
    )(asked, pool)


def attend_kernel(
    tensor_rows,
    place,
    length,
    queries,
    kv_new,
    pages,
    weight,
    give,
    keep,
    wide,
    wide_new,
    keys,
    values,
    blocks,
):
    dialogs, entries = place.shape
    rows = queries.shape[0]
    fresh = rows // dialogs
    heads = queries.shape[1] // HD
    block = rows // (2 * tensor_rows)
    width = weight.shape[1] // PANELS
    scale = 1.0 / math.sqrt(HD)
    nt = (((1,), (1,)), ((), ()))
    nn = (((1,), (0,)), ((), ()))
    wide_new[...] = kv_new[...].astype(jnp.float32)
    for dialog in range(dialogs):
        for entry in range(entries):
            wide[dialog, entry] = pages[place[dialog, entry]].astype(jnp.float32)
            span = slice(entry * PAGE, (entry + 1) * PAGE)
            keys[dialog, span, :] = wide[dialog, entry, pl.ds(0, PAGE, stride=2), :].astype(
                jnp.bfloat16
            )
            values[dialog, span, :] = wide[dialog, entry, pl.ds(1, PAGE, stride=2), :].astype(
                jnp.bfloat16
            )
    pieces = []
    for dialog in range(dialogs):
        own = slice(dialog * fresh, (dialog + 1) * fresh)
        asked = jnp.concatenate(
            [queries[own, head * HD : (head + 1) * HD] for head in range(heads)], axis=0
        )
        start = dialog * 2 * fresh
        keys_new = wide_new[pl.ds(start, fresh, stride=2), :].astype(jnp.bfloat16)
        values_new = wide_new[pl.ds(start + 1, fresh, stride=2), :].astype(jnp.bfloat16)
        score_new = (
            lax.dot_general(asked, keys_new, nt, preferred_element_type=jnp.float32) * scale
        )
        row = lax.broadcasted_iota(jnp.int32, score_new.shape, 0) % fresh
        col = lax.broadcasted_iota(jnp.int32, score_new.shape, 1)
        score_new = jnp.where(col <= row, score_new, FLOOR)
        score = lax.dot_general(asked, keys[dialog], nt, preferred_element_type=jnp.float32) * scale
        token = lax.broadcasted_iota(jnp.int32, score.shape, 1)
        score = jnp.where(token < length[dialog], score, FLOOR)
        peak = jnp.maximum(
            jnp.max(score, axis=1, keepdims=True), jnp.max(score_new, axis=1, keepdims=True)
        )
        part = jnp.exp(score - peak).astype(jnp.bfloat16)
        part_new = jnp.exp(score_new - peak).astype(jnp.bfloat16)
        amount = jnp.sum(part.astype(jnp.float32), axis=1, keepdims=True) + jnp.sum(
            part_new.astype(jnp.float32), axis=1, keepdims=True
        )
        summed = lax.dot_general(
            part, values[dialog], nn, preferred_element_type=jnp.float32
        ) + lax.dot_general(part_new, values_new, nn, preferred_element_type=jnp.float32)
        attended = summed / amount
        for head in range(heads):
            for index in range(fresh // block):
                first = head * fresh + index * block
                blocks[dialog * (fresh // block) + index, :, head * HD : (head + 1) * HD] = (
                    attended[first : first + block, :]
                )
    row, core = lax.axis_index("row"), lax.axis_index("core")
    across, beside = tensor_rows - 1 - row, row ^ 1
    orders = (
        (row, across, beside, across ^ 1),
        (row, beside, across, across ^ 1),
    )
    half = rows // 2
    sides = weight.shape[1] // len(orders)
    for side, order in enumerate(orders):
        mixed = jnp.concatenate(
            [blocks[2 * there + 1 - core] for there in order]
            + [blocks[2 * there + core] for there in order],
            axis=0,
        ).astype(jnp.bfloat16)
        for index in range(sides // width):
            number = side * (sides // width) + index
            span = slice(index * width, (index + 1) * width)
            product = lax.dot_general(
                mixed, weight[:, number * width : (number + 1) * width], nn, preferred_element_type=jnp.float32
            ).astype(jnp.bfloat16)
            give[side, :, span] = product[:half]
            keep[side, :, span] = product[half:]


def attend(place, hist_len, queries, kv_new, pages, weight, tensor_rows):
    dialogs, entries = place.shape
    rows = queries.shape[0]
    out = jax.ShapeDtypeStruct((2, rows // 2, weight.shape[1] // 2), jnp.bfloat16)
    smem = pl.BlockSpec(memory_space=pltpu.SMEM)
    vmem = pl.BlockSpec(memory_space=pltpu.VMEM)
    hbm = pl.BlockSpec(memory_space=pltpu.HBM)
    history = (dialogs, entries * PAGE, HD)
    return pl.pallas_call(
        functools.partial(attend_kernel, tensor_rows),
        out_shape=(out, out),
        in_specs=[smem, smem, vmem, vmem, vmem, vmem],
        out_specs=(vmem, vmem),
        scratch_shapes=[
            pltpu.VMEM((dialogs, entries) + pages.shape[1:], jnp.float32),
            pltpu.VMEM(kv_new.shape, jnp.float32),
            pltpu.VMEM(history, jnp.bfloat16),
            pltpu.VMEM(history, jnp.bfloat16),
            pltpu.VMEM((2 * tensor_rows, rows // (2 * tensor_rows), weight.shape[0]), jnp.float32),
        ],
        compiler_params=pltpu.CompilerParams(vmem_limit_bytes=24 * 1024 * 1024),
        name="attend",
    )(place, hist_len, queries, kv_new, pages, weight)


def sum_over_tensor(give, keep, tensor_rows):
    swap = [(0, 1), (1, 0)]
    beside = [(row, row ^ 1) for row in range(tensor_rows)]
    across = [(row, tensor_rows - 1 - row) for row in range(tensor_rows)]
    came = lax.ppermute(give, "core", swap)
    half = give.shape[1] // 2
    quarter = half // 2
    wide = jnp.float32
    near = keep[:, :half].astype(wide) + came[:, :half].astype(wide)
    far = (keep[:, half:].astype(wide) + came[:, half:].astype(wide)).astype(give.dtype)
    moved = (
        lax.ppermute(far[0], "row", beside),
        lax.ppermute(far[1], "row", across),
    )
    sums = [near[side] + moved[side].astype(wide) for side in range(2)]
    last = (
        lax.ppermute(sums[0][quarter:].astype(give.dtype), "row", across),
        lax.ppermute(sums[1][quarter:].astype(give.dtype), "row", beside),
    )
    return jnp.concatenate(
        [(sums[side][:quarter] + last[side].astype(wide)).astype(give.dtype) for side in range(2)],
        axis=1,
    )


def local(queries, kv_new, pool, page_table, hist_len, o_weight):
    groups = lax.axis_size(REPLICA)
    tensor_rows = lax.axis_size("row")
    shelves = pool.reshape(pool.shape[0], 2 * PAGE, HD)
    wanted, place = plan(page_table, hist_len, groups, pool.shape[0])
    asked = lax.all_to_all(wanted, REPLICA, split_axis=0, concat_axis=0, tiled=True)
    sent = collect(asked, shelves, groups)
    pages = lax.all_to_all(sent, REPLICA, split_axis=0, concat_axis=0, tiled=True)
    pages = pages.reshape(groups * SLOT, 2 * PAGE, HD)
    fresh = kv_new.reshape(2 * kv_new.shape[0], HD)
    give, keep = attend(place, hist_len, queries, fresh, pages, o_weight, tensor_rows)
    return sum_over_tensor(give, keep, tensor_rows)


def solution(mesh):
    split = Mesh(
        mesh.devices.reshape(4, 4, mesh.shape["tensor"] // 2, 2), REPLICA + TENSOR
    )
    in_specs = (
        P(REPLICA, TENSOR),
        P(REPLICA, None, TENSOR),
        P(REPLICA, None, None, TENSOR),
        P(REPLICA, None),
        P(REPLICA),
        P(TENSOR, None),
    )
    out_specs = P(REPLICA + TENSOR, None)
    return jax.shard_map(local, mesh=split, in_specs=in_specs, out_specs=out_specs, check_vma=False)
```

```python
import functools
import math

import jax
import jax.numpy as jnp
from jax import lax
from jax.experimental import pallas as pl
from jax.experimental.pallas import tpu as pltpu
from jax.sharding import Mesh
from jax.sharding import PartitionSpec as P

HD = 128
PAGE = 128
SLOT = 3
LANES = 128
PANELS = 8
SENDING = (2, 1, 3)
FLOOR = -1e30
REPLICA = ("replica_0", "replica_1")
TENSOR = ("row", "core")


def plan_kernel(groups, pool_size, table, length, wanted, place, count):
    dialogs, entries = table.shape
    for owner in range(groups):
        count[owner] = 0
        for slot in range(SLOT):
            wanted[owner, 0, slot] = 0
    for dialog in range(dialogs):
        tokens = length[dialog]
        for entry in range(entries):
            page = table[dialog, entry]
            owner = lax.div(page, pool_size)
            live = entry * PAGE < tokens
            rank = count[owner]

            @pl.when(live)
            def _():
                wanted[owner, 0, rank] = page - owner * pool_size
                count[owner] = rank + 1

            place[dialog, entry] = jnp.where(live, owner * SLOT + rank, 0)


def plan(page_table, hist_len, groups, pool_size):
    smem = pl.BlockSpec(memory_space=pltpu.SMEM)
    return pl.pallas_call(
        functools.partial(plan_kernel, groups, pool_size),
        out_shape=(
            jax.ShapeDtypeStruct((groups, 1, LANES), jnp.int32),
            jax.ShapeDtypeStruct(page_table.shape, jnp.int32),
        ),
        in_specs=[smem, smem],
        out_specs=(smem, smem),
        scratch_shapes=[pltpu.SMEM((groups,), jnp.int32)],
        compiler_params=pltpu.CompilerParams(vmem_limit_bytes=60000 * 1024),
        cost_estimate=pl.CostEstimate(flops=10**10, bytes_accessed=10**7, transcendentals=0),
        name="plan",
    )(page_table, hist_len)


def collect_kernel(groups, asked, pool, out, ids, ids_sem):
    read = pltpu.make_async_copy(asked, ids, ids_sem)
    read.start()
    read.wait()
    for owner in range(groups):
        for slot in range(SLOT):
            out[owner, slot] = pool[ids[owner, 0, slot]]


def collect(asked, pool, groups):
    shape = (groups, SLOT) + pool.shape[1:]
    vmem = pl.BlockSpec(memory_space=pltpu.VMEM)
    return pl.pallas_call(
        functools.partial(collect_kernel, groups),
        out_shape=jax.ShapeDtypeStruct(shape, pool.dtype),
        in_specs=[pl.BlockSpec(memory_space=pl.ANY), vmem],
        out_specs=vmem,
        scratch_shapes=[pltpu.SMEM(asked.shape, jnp.int32), pltpu.SemaphoreType.DMA],
        compiler_params=pltpu.CompilerParams(vmem_limit_bytes=8 * 1024 * 1024),
        cost_estimate=pl.CostEstimate(flops=100000000000, bytes_accessed=100000000, transcendentals=0),
        name="collect",
    )(asked, pool)


def attend_kernel(
    tensor_rows,
    place,
    length,
    queries,
    kv_new,
    pages,
    weight,
    give,
    keep,
    wide,
    wide_new,
    keys,
    values,
    blocks,
):
    dialogs, entries = place.shape
    rows = queries.shape[0]
    fresh = rows // dialogs
    heads = queries.shape[1] // HD
    block = rows // (2 * tensor_rows)
    width = weight.shape[1] // PANELS
    scale = 1.0 / math.sqrt(HD)
    nt = (((1,), (1,)), ((), ()))
    nn = (((1,), (0,)), ((), ()))
    wide_new[...] = kv_new[...].astype(jnp.float32)
    for dialog in range(dialogs):
        for entry in range(entries):
            wide[dialog, entry] = pages[place[dialog, entry]].astype(jnp.float32)
            span = slice(entry * PAGE, (entry + 1) * PAGE)
            keys[dialog, span, :] = wide[dialog, entry, pl.ds(0, PAGE, stride=2), :].astype(
                jnp.bfloat16
            )
            values[dialog, span, :] = wide[dialog, entry, pl.ds(1, PAGE, stride=2), :].astype(
                jnp.bfloat16
            )
    pieces = []
    for dialog in range(dialogs):
        own = slice(dialog * fresh, (dialog + 1) * fresh)
        asked = jnp.concatenate(
            [queries[own, head * HD : (head + 1) * HD] for head in range(heads)], axis=0
        )
        start = dialog * 2 * fresh
        keys_new = wide_new[pl.ds(start, fresh, stride=2), :].astype(jnp.bfloat16)
        values_new = wide_new[pl.ds(start + 1, fresh, stride=2), :].astype(jnp.bfloat16)
        score_new = (
            lax.dot_general(asked, keys_new, nt, preferred_element_type=jnp.float32) * scale
        )
        row = lax.broadcasted_iota(jnp.int32, score_new.shape, 0) % fresh
        col = lax.broadcasted_iota(jnp.int32, score_new.shape, 1)
        score_new = jnp.where(col <= row, score_new, FLOOR)
        score = lax.dot_general(asked, keys[dialog], nt, preferred_element_type=jnp.float32) * scale
        token = lax.broadcasted_iota(jnp.int32, score.shape, 1)
        score = jnp.where(token < length[dialog], score, FLOOR)
        peak = jnp.maximum(
            jnp.max(score, axis=1, keepdims=True), jnp.max(score_new, axis=1, keepdims=True)
        )
        part = jnp.exp(score - peak).astype(jnp.bfloat16)
        part_new = jnp.exp(score_new - peak).astype(jnp.bfloat16)
        amount = jnp.sum(part.astype(jnp.float32), axis=1, keepdims=True) + jnp.sum(
            part_new.astype(jnp.float32), axis=1, keepdims=True
        )
        summed = lax.dot_general(
            part, values[dialog], nn, preferred_element_type=jnp.float32
        ) + lax.dot_general(part_new, values_new, nn, preferred_element_type=jnp.float32)
        attended = summed / amount
        for head in range(heads):
            for index in range(fresh // block):
                first = head * fresh + index * block
                blocks[dialog * (fresh // block) + index, :, head * HD : (head + 1) * HD] = (
                    attended[first : first + block, :]
                )
    row, core = lax.axis_index("row"), lax.axis_index("core")
    order = [lax.rem(row + step, tensor_rows) for step in range(tensor_rows)]
    half = rows // 2
    mixed = jnp.concatenate(
        [blocks[2 * there + 1 - core] for there in order]
        + [blocks[2 * there + core] for there in order],
        axis=0,
    ).astype(jnp.bfloat16)
    for index in range(PANELS):
        span = slice(index * width, (index + 1) * width)
        product = lax.dot_general(
            mixed, weight[:, span], nn, preferred_element_type=jnp.float32
        ).astype(jnp.bfloat16)
        give[:, span] = product[:half]
        keep[:, span] = product[half:]


def attend(place, hist_len, queries, kv_new, pages, weight, tensor_rows):
    dialogs, entries = place.shape
    rows = queries.shape[0]
    out = jax.ShapeDtypeStruct((rows // 2, weight.shape[1]), jnp.bfloat16)
    smem = pl.BlockSpec(memory_space=pltpu.SMEM)
    vmem = pl.BlockSpec(memory_space=pltpu.VMEM)
    hbm = pl.BlockSpec(memory_space=pltpu.HBM)
    history = (dialogs, entries * PAGE, HD)
    return pl.pallas_call(
        functools.partial(attend_kernel, tensor_rows),
        out_shape=(out, out),
        in_specs=[smem, smem, vmem, vmem, vmem, vmem],
        out_specs=(vmem, vmem),
        scratch_shapes=[
            pltpu.VMEM((dialogs, entries) + pages.shape[1:], jnp.float32),
            pltpu.VMEM(kv_new.shape, jnp.float32),
            pltpu.VMEM(history, jnp.bfloat16),
            pltpu.VMEM(history, jnp.bfloat16),
            pltpu.VMEM((2 * tensor_rows, rows // (2 * tensor_rows), weight.shape[0]), jnp.float32),
        ],
        compiler_params=pltpu.CompilerParams(vmem_limit_bytes=24 * 1024 * 1024),
        name="attend",
    )(place, hist_len, queries, kv_new, pages, weight)


def sum_over_tensor(give, keep, tensor_rows):
    came = lax.ppermute(give, "core", [(0, 1), (1, 0)])
    block = give.shape[0] // tensor_rows
    wide = jnp.float32
    pair = [
        keep[step * block : (step + 1) * block].astype(wide)
        + came[step * block : (step + 1) * block].astype(wide)
        for step in range(tensor_rows)
    ]
    total = pair[0]
    for step in SENDING:
        turn = [(row, (row + step) % tensor_rows) for row in range(tensor_rows)]
        total = total + lax.ppermute(pair[step].astype(give.dtype), "row", turn).astype(wide)
    return total.astype(give.dtype)


def local(queries, kv_new, pool, page_table, hist_len, o_weight):
    groups = lax.axis_size(REPLICA)
    tensor_rows = lax.axis_size("row")
    shelves = pool.reshape(pool.shape[0], 2 * PAGE, HD)
    wanted, place = plan(page_table, hist_len, groups, pool.shape[0])
    asked = lax.all_to_all(wanted, REPLICA, split_axis=0, concat_axis=0, tiled=True)
    sent = collect(asked, shelves, groups)
    pages = lax.all_to_all(sent, REPLICA, split_axis=0, concat_axis=0, tiled=True)
    pages = pages.reshape(groups * SLOT, 2 * PAGE, HD)
    fresh = kv_new.reshape(2 * kv_new.shape[0], HD)
    give, keep = attend(place, hist_len, queries, fresh, pages, o_weight, tensor_rows)
    return sum_over_tensor(give, keep, tensor_rows)


def solution(mesh):
    split = Mesh(
        mesh.devices.reshape(4, 4, mesh.shape["tensor"] // 2, 2), REPLICA + TENSOR
    )
    in_specs = (
        P(REPLICA, TENSOR),
        P(REPLICA, None, TENSOR),
        P(REPLICA, None, None, TENSOR),
        P(REPLICA, None),
        P(REPLICA),
        P(TENSOR, None),
    )
    out_specs = P(REPLICA + TENSOR, None)
    return jax.shard_map(local, mesh=split, in_specs=in_specs, out_specs=out_specs, check_vma=False)
```

```python
import functools
import math

import jax
import jax.numpy as jnp
from jax import lax
from jax.experimental import pallas as pl
from jax.experimental.pallas import tpu as pltpu
from jax.sharding import Mesh
from jax.sharding import PartitionSpec as P

HD = 128
PAGE = 128
SLOT = 3
LANES = 128
PANELS = 8
SENDING = (2, 1, 3)
FLOOR = -1e30
SURE = 768
REPLICA = ("replica_0", "replica_1")
TENSOR = ("row", "core")


def plan_kernel(groups, pool_size, table, length, wanted, place, count):
    dialogs, entries = table.shape
    for owner in range(groups):
        count[owner] = 0
        for slot in range(SLOT):
            wanted[owner, 0, slot] = 0
    for dialog in range(dialogs):
        tokens = length[dialog]
        for entry in range(entries):
            page = table[dialog, entry]
            owner = lax.div(page, pool_size)
            live = entry * PAGE < tokens
            rank = count[owner]

            @pl.when(live)
            def _():
                wanted[owner, 0, rank] = page - owner * pool_size
                count[owner] = rank + 1

            place[dialog, entry] = jnp.where(live, owner * SLOT + rank, 0)


def plan(page_table, hist_len, groups, pool_size):
    smem = pl.BlockSpec(memory_space=pltpu.SMEM)
    return pl.pallas_call(
        functools.partial(plan_kernel, groups, pool_size),
        out_shape=(
            jax.ShapeDtypeStruct((groups, 1, LANES), jnp.int32),
            jax.ShapeDtypeStruct(page_table.shape, jnp.int32),
        ),
        in_specs=[smem, smem],
        out_specs=(smem, smem),
        scratch_shapes=[pltpu.SMEM((groups,), jnp.int32)],
        compiler_params=pltpu.CompilerParams(vmem_limit_bytes=60000 * 1024),
        cost_estimate=pl.CostEstimate(flops=10**10, bytes_accessed=10**7, transcendentals=0),
        name="plan",
    )(page_table, hist_len)


def collect_kernel(groups, asked, pool, out, ids, ids_sem):
    read = pltpu.make_async_copy(asked, ids, ids_sem)
    read.start()
    read.wait()
    for owner in range(groups):
        for slot in range(SLOT):
            out[owner, slot] = pool[ids[owner, 0, slot]]


def collect(asked, pool, groups):
    shape = (groups, SLOT) + pool.shape[1:]
    vmem = pl.BlockSpec(memory_space=pltpu.VMEM)
    return pl.pallas_call(
        functools.partial(collect_kernel, groups),
        out_shape=jax.ShapeDtypeStruct(shape, pool.dtype),
        in_specs=[pl.BlockSpec(memory_space=pl.ANY), vmem],
        out_specs=vmem,
        scratch_shapes=[pltpu.SMEM(asked.shape, jnp.int32), pltpu.SemaphoreType.DMA],
        compiler_params=pltpu.CompilerParams(vmem_limit_bytes=8 * 1024 * 1024),
        cost_estimate=pl.CostEstimate(flops=100000000000, bytes_accessed=100000000, transcendentals=0),
        name="collect",
    )(asked, pool)


def attend_kernel(
    tensor_rows,
    place,
    length,
    queries,
    kv_new,
    pages,
    weight,
    give,
    keep,
    wide,
    wide_new,
    keys,
    values,
    blocks,
):
    dialogs, entries = place.shape
    rows = queries.shape[0]
    fresh = rows // dialogs
    heads = queries.shape[1] // HD
    block = rows // (2 * tensor_rows)
    width = weight.shape[1] // PANELS
    rate = math.log2(math.e) / math.sqrt(HD)
    nt = (((1,), (1,)), ((), ()))
    nn = (((1,), (0,)), ((), ()))
    wide_new[...] = kv_new[...].astype(jnp.float32)
    for dialog in range(dialogs):
        values[dialog, :, HD:] = jnp.ones((entries * PAGE, HD), jnp.bfloat16)
        for entry in range(entries):
            wide[dialog, entry] = pages[place[dialog, entry]].astype(jnp.float32)
            span = slice(entry * PAGE, (entry + 1) * PAGE)
            keys[dialog, span, :] = wide[dialog, entry, pl.ds(0, PAGE, stride=2), :].astype(
                jnp.bfloat16
            )
            values[dialog, span, :HD] = wide[dialog, entry, pl.ds(1, PAGE, stride=2), :].astype(
                jnp.bfloat16
            )
    stage = []
    for dialog in range(dialogs):
        own = slice(dialog * fresh, (dialog + 1) * fresh)
        asked = jnp.concatenate(
            [queries[own, head * HD : (head + 1) * HD] for head in range(heads)], axis=0
        )
        start = dialog * 2 * fresh
        keys_new = wide_new[pl.ds(start, fresh, stride=2), :].astype(jnp.bfloat16)
        values_new = wide_new[pl.ds(start + 1, fresh, stride=2), :].astype(jnp.bfloat16)
        values_new = jnp.concatenate([values_new, jnp.ones_like(values_new)], axis=1)
        span = asked.shape[0] // 1
        for piece in range(1):
            some = asked[piece * span : (piece + 1) * span]
            score_new = lax.dot_general(some, keys_new, nt, preferred_element_type=jnp.float32)
            row = lax.broadcasted_iota(jnp.int32, score_new.shape, 0) % fresh
            col = lax.broadcasted_iota(jnp.int32, score_new.shape, 1)
            score_new = jnp.where(col <= row, score_new, FLOOR)
            score = lax.dot_general(some, keys[dialog], nt, preferred_element_type=jnp.float32)
            later = score[:, SURE:]
            token = SURE + lax.broadcasted_iota(jnp.int32, later.shape, 1)
            later = jnp.where(token < length[dialog], later, FLOOR)
            score = jnp.concatenate([score[:, :SURE], later], axis=1)
            stage.append((score, score_new, values_new))
    weights = []
    for score, score_new, values_new in stage:
        peak = jnp.maximum(
            jnp.max(score, axis=1, keepdims=True), jnp.max(score_new, axis=1, keepdims=True)
        )
        weights.append(
            (
                jnp.exp2((score - peak) * rate).astype(jnp.bfloat16),
                jnp.exp2((score_new - peak) * rate).astype(jnp.bfloat16),
                values_new,
            )
        )
    for dialog in range(dialogs):
        parts = []
        for piece in range(1):
            part, part_new, values_new = weights[dialog * 1 + piece]
            summed = lax.dot_general(
                part, values[dialog], nn, preferred_element_type=jnp.float32
            ) + lax.dot_general(part_new, values_new, nn, preferred_element_type=jnp.float32)
            parts.append(summed[:, :HD] / summed[:, HD:])
        attended = jnp.concatenate(parts, axis=0)
        for head in range(heads):
            for index in range(fresh // block):
                first = head * fresh + index * block
                blocks[dialog * (fresh // block) + index, :, head * HD : (head + 1) * HD] = (
                    attended[first : first + block, :]
                )
    row, core = lax.axis_index("row"), lax.axis_index("core")
    order = [lax.rem(row + step, tensor_rows) for step in range(tensor_rows)]
    half = rows // 2
    mixed = jnp.concatenate(
        [blocks[2 * there + 1 - core] for there in order]
        + [blocks[2 * there + core] for there in order],
        axis=0,
    ).astype(jnp.bfloat16)
    for index in range(PANELS):
        span = slice(index * width, (index + 1) * width)
        product = lax.dot_general(
            mixed, weight[:, span], nn, preferred_element_type=jnp.float32
        ).astype(jnp.bfloat16)
        give[:, span] = product[:half]
        keep[:, span] = product[half:]


def attend(place, hist_len, queries, kv_new, pages, weight, tensor_rows):
    dialogs, entries = place.shape
    rows = queries.shape[0]
    out = jax.ShapeDtypeStruct((rows // 2, weight.shape[1]), jnp.bfloat16)
    smem = pl.BlockSpec(memory_space=pltpu.SMEM)
    vmem = pl.BlockSpec(memory_space=pltpu.VMEM)
    hbm = pl.BlockSpec(memory_space=pltpu.HBM)
    history = (dialogs, entries * PAGE, HD)
    return pl.pallas_call(
        functools.partial(attend_kernel, tensor_rows),
        out_shape=(out, out),
        in_specs=[smem, smem, vmem, vmem, vmem, vmem],
        out_specs=(vmem, vmem),
        scratch_shapes=[
            pltpu.VMEM((dialogs, entries) + pages.shape[1:], jnp.float32),
            pltpu.VMEM(kv_new.shape, jnp.float32),
            pltpu.VMEM(history, jnp.bfloat16),
            pltpu.VMEM(history[:2] + (2 * HD,), jnp.bfloat16),
            pltpu.VMEM((2 * tensor_rows, rows // (2 * tensor_rows), weight.shape[0]), jnp.float32),
        ],
        compiler_params=pltpu.CompilerParams(vmem_limit_bytes=24 * 1024 * 1024),
        name="attend",
    )(place, hist_len, queries, kv_new, pages, weight)


def sum_over_tensor(give, keep, tensor_rows):
    came = lax.ppermute(give, "core", [(0, 1), (1, 0)])
    block = give.shape[0] // tensor_rows
    wide = jnp.float32
    pair = [
        keep[step * block : (step + 1) * block].astype(wide)
        + came[step * block : (step + 1) * block].astype(wide)
        for step in range(tensor_rows)
    ]
    total = pair[0]
    for step in SENDING:
        turn = [(row, (row + step) % tensor_rows) for row in range(tensor_rows)]
        total = total + lax.ppermute(pair[step].astype(give.dtype), "row", turn).astype(wide)
    return total.astype(give.dtype)


def local(queries, kv_new, pool, page_table, hist_len, o_weight):
    groups = lax.axis_size(REPLICA)
    tensor_rows = lax.axis_size("row")
    shelves = pool.reshape(pool.shape[0], 2 * PAGE, HD)
    wanted, place = plan(page_table, hist_len, groups, pool.shape[0])
    asked = lax.all_to_all(wanted, REPLICA, split_axis=0, concat_axis=0, tiled=True)
    sent = collect(asked, shelves, groups)
    pages = lax.all_to_all(sent, REPLICA, split_axis=0, concat_axis=0, tiled=True)
    pages = pages.reshape(groups * SLOT, 2 * PAGE, HD)
    fresh = kv_new.reshape(2 * kv_new.shape[0], HD)
    give, keep = attend(place, hist_len, queries, fresh, pages, o_weight, tensor_rows)
    return sum_over_tensor(give, keep, tensor_rows)


def solution(mesh):
    split = Mesh(
        mesh.devices.reshape(4, 4, mesh.shape["tensor"] // 2, 2), REPLICA + TENSOR
    )
    in_specs = (
        P(REPLICA, TENSOR),
        P(REPLICA, None, TENSOR),
        P(REPLICA, None, None, TENSOR),
        P(REPLICA, None),
        P(REPLICA),
        P(TENSOR, None),
    )
    out_specs = P(REPLICA + TENSOR, None)
    return jax.shard_map(local, mesh=split, in_specs=in_specs, out_specs=out_specs, check_vma=False)
```

```python
import functools
import math

import jax
import jax.numpy as jnp
from jax import lax
from jax.experimental import pallas as pl
from jax.experimental.pallas import tpu as pltpu
from jax.sharding import Mesh
from jax.sharding import PartitionSpec as P

HD = 128
PAGE = 128
SLOT = 3
LANES = 128
PANELS = 8
SENDING = (2, 1, 3)
CODE = 256
PIECES = 4
FLOOR = -1e30
SURE = 768
REPLICA = ("replica_0", "replica_1")
TENSOR = ("row", "core")


def plan_kernel(groups, pool_size, table, length, wanted, place, count):
    dialogs, entries = table.shape
    for owner in range(groups):
        count[owner] = 0
        for slot in range(SLOT):
            wanted[owner, 0, slot] = 0
    for dialog in range(dialogs):
        tokens = length[dialog]
        for entry in range(entries):
            page = table[dialog, entry]
            owner = lax.div(page, pool_size)
            live = entry * PAGE < tokens
            rank = count[owner]

            @pl.when(live)
            def _():
                fill = jnp.minimum(tokens - entry * PAGE, PAGE)
                wanted[owner, 0, rank] = (page - owner * pool_size) * CODE + fill
                count[owner] = rank + 1

            place[dialog, entry] = jnp.where(live, owner * SLOT + rank, 0)


def plan(page_table, hist_len, groups, pool_size):
    smem = pl.BlockSpec(memory_space=pltpu.SMEM)
    return pl.pallas_call(
        functools.partial(plan_kernel, groups, pool_size),
        out_shape=(
            jax.ShapeDtypeStruct((groups, 1, LANES), jnp.int32),
            jax.ShapeDtypeStruct(page_table.shape, jnp.int32),
        ),
        in_specs=[smem, smem],
        out_specs=(smem, smem),
        scratch_shapes=[pltpu.SMEM((groups,), jnp.int32)],
        compiler_params=pltpu.CompilerParams(vmem_limit_bytes=60000 * 1024),
        cost_estimate=pl.CostEstimate(flops=10**10, bytes_accessed=10**7, transcendentals=0),
        name="plan",
    )(page_table, hist_len)


def collect_kernel(groups, asked, pool, out, ids, ids_sem):
    read = pltpu.make_async_copy(asked, ids, ids_sem)
    read.start()
    read.wait()
    piece = pool.shape[1] // PIECES
    for owner in range(groups):
        for slot in range(SLOT):
            code = ids[owner, 0, slot]
            shelf, fill = code // CODE, code % CODE
            for index in range(PIECES):
                span = slice(index * piece, (index + 1) * piece)
                block = pool[shelf, span, :]
                used = fill > index * (PAGE // PIECES)
                out[owner, slot, span, :] = jnp.where(used, block, jnp.zeros_like(block))


def collect(asked, pool, groups):
    shape = (groups, SLOT) + pool.shape[1:]
    vmem = pl.BlockSpec(memory_space=pltpu.VMEM)
    return pl.pallas_call(
        functools.partial(collect_kernel, groups),
        out_shape=jax.ShapeDtypeStruct(shape, pool.dtype),
        in_specs=[pl.BlockSpec(memory_space=pl.ANY), vmem],
        out_specs=vmem,
        scratch_shapes=[pltpu.SMEM(asked.shape, jnp.int32), pltpu.SemaphoreType.DMA],
        compiler_params=pltpu.CompilerParams(vmem_limit_bytes=8 * 1024 * 1024),
        cost_estimate=pl.CostEstimate(flops=100000000000, bytes_accessed=100000000, transcendentals=0),
        name="collect",
    )(asked, pool)


def attend_kernel(
    tensor_rows,
    place,
    length,
    queries,
    kv_new,
    pages,
    weight,
    give,
    keep,
    wide,
    wide_new,
    keys,
    values,
    blocks,
):
    dialogs, entries = place.shape
    rows = queries.shape[0]
    fresh = rows // dialogs
    heads = queries.shape[1] // HD
    block = rows // (2 * tensor_rows)
    width = weight.shape[1] // PANELS
    rate = math.log2(math.e) / math.sqrt(HD)
    nt = (((1,), (1,)), ((), ()))
    nn = (((1,), (0,)), ((), ()))
    wide_new[...] = kv_new[...].astype(jnp.float32)
    for dialog in range(dialogs):
        values[dialog, :, HD:] = jnp.ones((entries * PAGE, HD), jnp.bfloat16)
        for entry in range(entries):
            wide[dialog, entry] = pages[place[dialog, entry]].astype(jnp.float32)
            span = slice(entry * PAGE, (entry + 1) * PAGE)
            keys[dialog, span, :] = wide[dialog, entry, pl.ds(0, PAGE, stride=2), :].astype(
                jnp.bfloat16
            )
            values[dialog, span, :HD] = wide[dialog, entry, pl.ds(1, PAGE, stride=2), :].astype(
                jnp.bfloat16
            )
    stage = []
    for dialog in range(dialogs):
        own = slice(dialog * fresh, (dialog + 1) * fresh)
        asked = jnp.concatenate(
            [queries[own, head * HD : (head + 1) * HD] for head in range(heads)], axis=0
        )
        start = dialog * 2 * fresh
        keys_new = wide_new[pl.ds(start, fresh, stride=2), :].astype(jnp.bfloat16)
        values_new = wide_new[pl.ds(start + 1, fresh, stride=2), :].astype(jnp.bfloat16)
        values_new = jnp.concatenate([values_new, jnp.ones_like(values_new)], axis=1)
        span = asked.shape[0] // 1
        for piece in range(1):
            some = asked[piece * span : (piece + 1) * span]
            score_new = lax.dot_general(some, keys_new, nt, preferred_element_type=jnp.float32)
            row = lax.broadcasted_iota(jnp.int32, score_new.shape, 0) % fresh
            col = lax.broadcasted_iota(jnp.int32, score_new.shape, 1)
            score_new = jnp.where(col <= row, score_new, FLOOR)
            score = lax.dot_general(some, keys[dialog], nt, preferred_element_type=jnp.float32)
            later = score[:, SURE:]
            token = SURE + lax.broadcasted_iota(jnp.int32, later.shape, 1)
            later = jnp.where(token < length[dialog], later, FLOOR)
            score = jnp.concatenate([score[:, :SURE], later], axis=1)
            stage.append((score, score_new, values_new))
    weights = []
    for score, score_new, values_new in stage:
        peak = jnp.maximum(
            jnp.max(score, axis=1, keepdims=True), jnp.max(score_new, axis=1, keepdims=True)
        )
        weights.append(
            (
                jnp.exp2((score - peak) * rate).astype(jnp.bfloat16),
                jnp.exp2((score_new - peak) * rate).astype(jnp.bfloat16),
                values_new,
            )
        )
    for dialog in range(dialogs):
        parts = []
        for piece in range(1):
            part, part_new, values_new = weights[dialog * 1 + piece]
            summed = lax.dot_general(
                part, values[dialog], nn, preferred_element_type=jnp.float32
            ) + lax.dot_general(part_new, values_new, nn, preferred_element_type=jnp.float32)
            parts.append(summed[:, :HD] / summed[:, HD:])
        attended = jnp.concatenate(parts, axis=0)
        for head in range(heads):
            for index in range(fresh // block):
                first = head * fresh + index * block
                blocks[dialog * (fresh // block) + index, :, head * HD : (head + 1) * HD] = (
                    attended[first : first + block, :]
                )
    row, core = lax.axis_index("row"), lax.axis_index("core")
    order = [lax.rem(row + step, tensor_rows) for step in range(tensor_rows)]
    half = rows // 2
    mixed = jnp.concatenate(
        [blocks[2 * there + 1 - core] for there in order]
        + [blocks[2 * there + core] for there in order],
        axis=0,
    ).astype(jnp.bfloat16)
    for index in range(PANELS):
        span = slice(index * width, (index + 1) * width)
        product = lax.dot_general(
            mixed, weight[:, span], nn, preferred_element_type=jnp.float32
        ).astype(jnp.bfloat16)
        give[:, span] = product[:half]
        keep[:, span] = product[half:]


def attend(place, hist_len, queries, kv_new, pages, weight, tensor_rows):
    dialogs, entries = place.shape
    rows = queries.shape[0]
    out = jax.ShapeDtypeStruct((rows // 2, weight.shape[1]), jnp.bfloat16)
    smem = pl.BlockSpec(memory_space=pltpu.SMEM)
    vmem = pl.BlockSpec(memory_space=pltpu.VMEM)
    hbm = pl.BlockSpec(memory_space=pltpu.HBM)
    history = (dialogs, entries * PAGE, HD)
    return pl.pallas_call(
        functools.partial(attend_kernel, tensor_rows),
        out_shape=(out, out),
        in_specs=[smem, smem, vmem, vmem, vmem, vmem],
        out_specs=(vmem, vmem),
        scratch_shapes=[
            pltpu.VMEM((dialogs, entries) + pages.shape[1:], jnp.float32),
            pltpu.VMEM(kv_new.shape, jnp.float32),
            pltpu.VMEM(history, jnp.bfloat16),
            pltpu.VMEM(history[:2] + (2 * HD,), jnp.bfloat16),
            pltpu.VMEM((2 * tensor_rows, rows // (2 * tensor_rows), weight.shape[0]), jnp.float32),
        ],
        compiler_params=pltpu.CompilerParams(vmem_limit_bytes=24 * 1024 * 1024),
        name="attend",
    )(place, hist_len, queries, kv_new, pages, weight)


def sum_over_tensor(give, keep, tensor_rows):
    came = lax.ppermute(give, "core", [(0, 1), (1, 0)])
    block = give.shape[0] // tensor_rows
    wide = jnp.float32
    pair = [
        keep[step * block : (step + 1) * block].astype(wide)
        + came[step * block : (step + 1) * block].astype(wide)
        for step in range(tensor_rows)
    ]
    total = pair[0]
    for step in SENDING:
        turn = [(row, (row + step) % tensor_rows) for row in range(tensor_rows)]
        total = total + lax.ppermute(pair[step].astype(give.dtype), "row", turn).astype(wide)
    return total.astype(give.dtype)


def local(queries, kv_new, pool, page_table, hist_len, o_weight):
    groups = lax.axis_size(REPLICA)
    tensor_rows = lax.axis_size("row")
    shelves = pool.reshape(pool.shape[0], 2 * PAGE, HD)
    wanted, place = plan(page_table, hist_len, groups, pool.shape[0])
    asked = lax.all_to_all(wanted, REPLICA, split_axis=0, concat_axis=0, tiled=True)
    sent = collect(asked, shelves, groups)
    pages = lax.all_to_all(sent, REPLICA, split_axis=0, concat_axis=0, tiled=True)
    pages = pages.reshape(groups * SLOT, 2 * PAGE, HD)
    fresh = kv_new.reshape(2 * kv_new.shape[0], HD)
    give, keep = attend(place, hist_len, queries, fresh, pages, o_weight, tensor_rows)
    return sum_over_tensor(give, keep, tensor_rows)


def solution(mesh):
    split = Mesh(
        mesh.devices.reshape(4, 4, mesh.shape["tensor"] // 2, 2), REPLICA + TENSOR
    )
    in_specs = (
        P(REPLICA, TENSOR),
        P(REPLICA, None, TENSOR),
        P(REPLICA, None, None, TENSOR),
        P(REPLICA, None),
        P(REPLICA),
        P(TENSOR, None),
    )
    out_specs = P(REPLICA + TENSOR, None)
    return jax.shard_map(local, mesh=split, in_specs=in_specs, out_specs=out_specs, check_vma=False)
```

```python
import functools
import math

import jax
import jax.numpy as jnp
from jax import lax
from jax.experimental import pallas as pl
from jax.experimental.pallas import tpu as pltpu
from jax.sharding import Mesh
from jax.sharding import PartitionSpec as P

HD = 128
PAGE = 128
SLOT = 3
LANES = 128
PANELS = 8
SENDING = (2, 1, 3)
FLOOR = -1e30
SURE = 768
REPLICA = ("replica_0", "replica_1")
TENSOR = ("row", "core")


def plan_kernel(groups, pool_size, table, length, wanted, place, count):
    dialogs, entries = table.shape
    for owner in range(groups):
        count[owner] = 0
        for slot in range(SLOT):
            wanted[owner, 0, slot] = 0
    for dialog in range(dialogs):
        tokens = length[dialog]
        place[dialog, entries] = tokens
        for entry in range(entries):
            page = table[dialog, entry]
            owner = lax.div(page, pool_size)
            live = entry * PAGE < tokens
            rank = count[owner]

            @pl.when(live)
            def _():
                wanted[owner, 0, rank] = page - owner * pool_size
                count[owner] = rank + 1

            place[dialog, entry] = jnp.where(live, owner * SLOT + rank, 0)


def plan(page_table, hist_len, groups, pool_size):
    smem = pl.BlockSpec(memory_space=pltpu.SMEM)
    return pl.pallas_call(
        functools.partial(plan_kernel, groups, pool_size),
        out_shape=(
            jax.ShapeDtypeStruct((groups, 1, LANES), jnp.int32),
            jax.ShapeDtypeStruct((page_table.shape[0], page_table.shape[1] + 1), jnp.int32),
        ),
        in_specs=[smem, smem],
        out_specs=(smem, smem),
        scratch_shapes=[pltpu.SMEM((groups,), jnp.int32)],
        compiler_params=pltpu.CompilerParams(vmem_limit_bytes=60000 * 1024),
        cost_estimate=pl.CostEstimate(flops=10**10, bytes_accessed=10**7, transcendentals=0),
        name="plan",
    )(page_table, hist_len)


def collect_kernel(groups, asked, pool, out, ids, ids_sem):
    read = pltpu.make_async_copy(asked, ids, ids_sem)
    read.start()
    read.wait()
    for owner in range(groups):
        for slot in range(SLOT):
            out[owner, slot] = pool[ids[owner, 0, slot]]


def collect(asked, pool, groups):
    shape = (groups, SLOT) + pool.shape[1:]
    vmem = pl.BlockSpec(memory_space=pltpu.VMEM)
    return pl.pallas_call(
        functools.partial(collect_kernel, groups),
        out_shape=jax.ShapeDtypeStruct(shape, pool.dtype),
        in_specs=[pl.BlockSpec(memory_space=pl.ANY), vmem],
        out_specs=vmem,
        scratch_shapes=[pltpu.SMEM(asked.shape, jnp.int32), pltpu.SemaphoreType.DMA],
        compiler_params=pltpu.CompilerParams(vmem_limit_bytes=8 * 1024 * 1024),
        cost_estimate=pl.CostEstimate(flops=100000000000, bytes_accessed=100000000, transcendentals=0),
        name="collect",
    )(asked, pool)


def attend_kernel(
    tensor_rows,
    place,
    queries,
    kv_new,
    pages,
    weight,
    give,
    keep,
    wide,
    wide_new,
    keys,
    values,
    blocks,
):
    dialogs, entries = place.shape[0], place.shape[1] - 1
    rows = queries.shape[0]
    fresh = rows // dialogs
    heads = queries.shape[1] // HD
    block = rows // (2 * tensor_rows)
    width = weight.shape[1] // PANELS
    rate = math.log2(math.e) / math.sqrt(HD)
    nt = (((1,), (1,)), ((), ()))
    nn = (((1,), (0,)), ((), ()))
    wide_new[...] = kv_new[...].astype(jnp.float32)
    for dialog in range(dialogs):
        values[dialog, :, HD:] = jnp.ones((entries * PAGE, HD), jnp.bfloat16)
        for entry in range(entries):
            wide[dialog, entry] = pages[place[dialog, entry]].astype(jnp.float32)
            span = slice(entry * PAGE, (entry + 1) * PAGE)
            keys[dialog, span, :] = wide[dialog, entry, pl.ds(0, PAGE, stride=2), :].astype(
                jnp.bfloat16
            )
            values[dialog, span, :HD] = wide[dialog, entry, pl.ds(1, PAGE, stride=2), :].astype(
                jnp.bfloat16
            )
    stage = []
    for dialog in range(dialogs):
        own = slice(dialog * fresh, (dialog + 1) * fresh)
        asked = jnp.concatenate(
            [queries[own, head * HD : (head + 1) * HD] for head in range(heads)], axis=0
        )
        start = dialog * 2 * fresh
        keys_new = wide_new[pl.ds(start, fresh, stride=2), :].astype(jnp.bfloat16)
        values_new = wide_new[pl.ds(start + 1, fresh, stride=2), :].astype(jnp.bfloat16)
        values_new = jnp.concatenate([values_new, jnp.ones_like(values_new)], axis=1)
        span = asked.shape[0] // 1
        for piece in range(1):
            some = asked[piece * span : (piece + 1) * span]
            score_new = lax.dot_general(some, keys_new, nt, preferred_element_type=jnp.float32)
            row = lax.broadcasted_iota(jnp.int32, score_new.shape, 0) % fresh
            col = lax.broadcasted_iota(jnp.int32, score_new.shape, 1)
            score_new = jnp.where(col <= row, score_new, FLOOR)
            score = lax.dot_general(some, keys[dialog], nt, preferred_element_type=jnp.float32)
            later = score[:, SURE:]
            token = SURE + lax.broadcasted_iota(jnp.int32, later.shape, 1)
            later = jnp.where(token < place[dialog, entries], later, FLOOR)
            score = jnp.concatenate([score[:, :SURE], later], axis=1)
            stage.append((score, score_new, values_new))
    weights = []
    for score, score_new, values_new in stage:
        peak = jnp.maximum(
            jnp.max(score, axis=1, keepdims=True), jnp.max(score_new, axis=1, keepdims=True)
        )
        weights.append(
            (
                jnp.exp2((score - peak) * rate).astype(jnp.bfloat16),
                jnp.exp2((score_new - peak) * rate).astype(jnp.bfloat16),
                values_new,
            )
        )
    for dialog in range(dialogs):
        parts = []
        for piece in range(1):
            part, part_new, values_new = weights[dialog * 1 + piece]
            summed = lax.dot_general(
                part, values[dialog], nn, preferred_element_type=jnp.float32
            ) + lax.dot_general(part_new, values_new, nn, preferred_element_type=jnp.float32)
            parts.append(summed[:, :HD] / summed[:, HD:])
        attended = jnp.concatenate(parts, axis=0)
        for head in range(heads):
            for index in range(fresh // block):
                first = head * fresh + index * block
                blocks[dialog * (fresh // block) + index, :, head * HD : (head + 1) * HD] = (
                    attended[first : first + block, :]
                )
    row, core = lax.axis_index("row"), lax.axis_index("core")
    order = [lax.rem(row + step, tensor_rows) for step in range(tensor_rows)]
    half = rows // 2
    mixed = jnp.concatenate(
        [blocks[2 * there + 1 - core] for there in order]
        + [blocks[2 * there + core] for there in order],
        axis=0,
    ).astype(jnp.bfloat16)
    for index in range(PANELS):
        span = slice(index * width, (index + 1) * width)
        product = lax.dot_general(
            mixed, weight[:, span], nn, preferred_element_type=jnp.float32
        ).astype(jnp.bfloat16)
        give[:, span] = product[:half]
        keep[:, span] = product[half:]


def attend(place, queries, kv_new, pages, weight, tensor_rows):
    dialogs, entries = place.shape[0], place.shape[1] - 1
    rows = queries.shape[0]
    out = jax.ShapeDtypeStruct((rows // 2, weight.shape[1]), jnp.bfloat16)
    smem = pl.BlockSpec(memory_space=pltpu.SMEM)
    vmem = pl.BlockSpec(memory_space=pltpu.VMEM)
    hbm = pl.BlockSpec(memory_space=pltpu.HBM)
    history = (dialogs, entries * PAGE, HD)
    return pl.pallas_call(
        functools.partial(attend_kernel, tensor_rows),
        out_shape=(out, out),
        in_specs=[smem, vmem, vmem, vmem, vmem],
        out_specs=(vmem, vmem),
        scratch_shapes=[
            pltpu.VMEM((dialogs, entries) + pages.shape[1:], jnp.float32),
            pltpu.VMEM(kv_new.shape, jnp.float32),
            pltpu.VMEM(history, jnp.bfloat16),
            pltpu.VMEM(history[:2] + (2 * HD,), jnp.bfloat16),
            pltpu.VMEM((2 * tensor_rows, rows // (2 * tensor_rows), weight.shape[0]), jnp.float32),
        ],
        compiler_params=pltpu.CompilerParams(vmem_limit_bytes=24 * 1024 * 1024),
        name="attend",
    )(place, queries, kv_new, pages, weight)


def sum_over_tensor(give, keep, tensor_rows):
    came = lax.ppermute(give, "core", [(0, 1), (1, 0)])
    block = give.shape[0] // tensor_rows
    wide = jnp.float32
    pair = [
        keep[step * block : (step + 1) * block].astype(wide)
        + came[step * block : (step + 1) * block].astype(wide)
        for step in range(tensor_rows)
    ]
    total = pair[0]
    sent = lax.optimization_barrier(tuple(pair[step].astype(give.dtype) for step in SENDING))
    for step, block in zip(SENDING, sent):
        turn = [(row, (row + step) % tensor_rows) for row in range(tensor_rows)]
        total = total + lax.ppermute(block, "row", turn).astype(wide)
    return total.astype(give.dtype)


def local(queries, kv_new, pool, page_table, hist_len, o_weight):
    groups = lax.axis_size(REPLICA)
    tensor_rows = lax.axis_size("row")
    shelves = pool.reshape(pool.shape[0], 2 * PAGE, HD)
    wanted, place = plan(page_table, hist_len, groups, pool.shape[0])
    asked = lax.all_to_all(wanted, REPLICA, split_axis=0, concat_axis=0, tiled=True)
    sent = collect(asked, shelves, groups)
    pages = lax.all_to_all(sent, REPLICA, split_axis=0, concat_axis=0, tiled=True)
    pages = pages.reshape(groups * SLOT, 2 * PAGE, HD)
    fresh = kv_new.reshape(2 * kv_new.shape[0], HD)
    give, keep = attend(place, queries, fresh, pages, o_weight, tensor_rows)
    return sum_over_tensor(give, keep, tensor_rows)


def solution(mesh):
    split = Mesh(
        mesh.devices.reshape(4, 4, mesh.shape["tensor"] // 2, 2), REPLICA + TENSOR
    )
    in_specs = (
        P(REPLICA, TENSOR),
        P(REPLICA, None, TENSOR),
        P(REPLICA, None, None, TENSOR),
        P(REPLICA, None),
        P(REPLICA),
        P(TENSOR, None),
    )
    out_specs = P(REPLICA + TENSOR, None)
    return jax.shard_map(local, mesh=split, in_specs=in_specs, out_specs=out_specs, check_vma=False)
```

```python
import functools
import math

import jax
import jax.numpy as jnp
from jax import lax
from jax.experimental import pallas as pl
from jax.experimental.pallas import tpu as pltpu
from jax.sharding import Mesh
from jax.sharding import PartitionSpec as P

HD = 128
PAGE = 128
SLOT = 3
LANES = 128
PANELS = 8
SENDING = (2, 1, 3)
FLOOR = -1e30
SURE = 768
REPLICA = ("replica_0", "replica_1")
TENSOR = ("row", "core")


def plan_kernel(groups, pool_size, table, length, wanted, place, count):
    dialogs, entries = table.shape
    for owner in range(groups):
        count[owner] = 0
        for slot in range(SLOT):
            wanted[owner, 0, slot] = 0
    for dialog in range(dialogs):
        tokens = length[dialog]
        for entry in range(entries):
            page = table[dialog, entry]
            owner = lax.div(page, pool_size)
            live = entry * PAGE < tokens
            rank = count[owner]

            @pl.when(live)
            def _():
                wanted[owner, 0, rank] = page - owner * pool_size
                count[owner] = rank + 1

            place[dialog, entry] = jnp.where(live, owner * SLOT + rank, 0)


def plan(page_table, hist_len, groups, pool_size):
    smem = pl.BlockSpec(memory_space=pltpu.SMEM)
    return pl.pallas_call(
        functools.partial(plan_kernel, groups, pool_size),
        out_shape=(
            jax.ShapeDtypeStruct((groups, 1, LANES), jnp.int32),
            jax.ShapeDtypeStruct(page_table.shape, jnp.int32),
        ),
        in_specs=[smem, smem],
        out_specs=(smem, smem),
        scratch_shapes=[pltpu.SMEM((groups,), jnp.int32)],
        compiler_params=pltpu.CompilerParams(vmem_limit_bytes=60000 * 1024),
        cost_estimate=pl.CostEstimate(flops=10**10, bytes_accessed=10**7, transcendentals=0),
        name="plan",
    )(page_table, hist_len)


def collect_kernel(groups, asked, pool, out, ids, ids_sem):
    read = pltpu.make_async_copy(asked, ids, ids_sem)
    read.start()
    read.wait()
    for owner in range(groups):
        for slot in range(SLOT):
            out[owner, slot] = pool[ids[owner, 0, slot]]


def collect(asked, pool, groups):
    shape = (groups, SLOT) + pool.shape[1:]
    vmem = pl.BlockSpec(memory_space=pltpu.VMEM)
    return pl.pallas_call(
        functools.partial(collect_kernel, groups),
        out_shape=jax.ShapeDtypeStruct(shape, pool.dtype),
        in_specs=[pl.BlockSpec(memory_space=pl.ANY), vmem],
        out_specs=vmem,
        scratch_shapes=[pltpu.SMEM(asked.shape, jnp.int32), pltpu.SemaphoreType.DMA],
        compiler_params=pltpu.CompilerParams(vmem_limit_bytes=8 * 1024 * 1024),
        cost_estimate=pl.CostEstimate(flops=100000000000, bytes_accessed=100000000, transcendentals=0),
        name="collect",
    )(asked, pool)


def attend_kernel(
    tensor_rows,
    place,
    length,
    queries,
    kv_new,
    pages,
    weight,
    give,
    keep,
    wide,
    wide_new,
    keys,
    values,
    blocks,
):
    dialogs, entries = place.shape
    rows = queries.shape[0]
    fresh = rows // dialogs
    heads = queries.shape[1] // HD
    block = rows // (2 * tensor_rows)
    width = weight.shape[1] // PANELS
    rate = math.log2(math.e) / math.sqrt(HD)
    nt = (((1,), (1,)), ((), ()))
    nn = (((1,), (0,)), ((), ()))
    wide_new[...] = kv_new[...].astype(jnp.float32)
    stage = []
    for dialog in range(dialogs):
        values[dialog, :, HD:] = jnp.ones((entries * PAGE, HD), jnp.bfloat16)
        for entry in range(entries):
            wide[dialog, entry] = pages[place[dialog, entry]].astype(jnp.float32)
            span = slice(entry * PAGE, (entry + 1) * PAGE)
            keys[dialog, span, :] = wide[dialog, entry, pl.ds(0, PAGE, stride=2), :].astype(
                jnp.bfloat16
            )
            values[dialog, span, :HD] = wide[dialog, entry, pl.ds(1, PAGE, stride=2), :].astype(
                jnp.bfloat16
            )
        own = slice(dialog * fresh, (dialog + 1) * fresh)
        asked = jnp.concatenate(
            [queries[own, head * HD : (head + 1) * HD] for head in range(heads)], axis=0
        )
        start = dialog * 2 * fresh
        keys_new = wide_new[pl.ds(start, fresh, stride=2), :].astype(jnp.bfloat16)
        values_new = wide_new[pl.ds(start + 1, fresh, stride=2), :].astype(jnp.bfloat16)
        values_new = jnp.concatenate([values_new, jnp.ones_like(values_new)], axis=1)
        span = asked.shape[0] // 1
        for piece in range(1):
            some = asked[piece * span : (piece + 1) * span]
            score_new = lax.dot_general(some, keys_new, nt, preferred_element_type=jnp.float32)
            row = lax.broadcasted_iota(jnp.int32, score_new.shape, 0) % fresh
            col = lax.broadcasted_iota(jnp.int32, score_new.shape, 1)
            score_new = jnp.where(col <= row, score_new, FLOOR)
            score = lax.dot_general(some, keys[dialog], nt, preferred_element_type=jnp.float32)
            later = score[:, SURE:]
            token = SURE + lax.broadcasted_iota(jnp.int32, later.shape, 1)
            later = jnp.where(token < length[dialog], later, FLOOR)
            score = jnp.concatenate([score[:, :SURE], later], axis=1)
            stage.append((score, score_new, values_new))
    weights = []
    for score, score_new, values_new in stage:
        peak = jnp.maximum(
            jnp.max(score, axis=1, keepdims=True), jnp.max(score_new, axis=1, keepdims=True)
        )
        weights.append(
            (
                jnp.exp2((score - peak) * rate).astype(jnp.bfloat16),
                jnp.exp2((score_new - peak) * rate).astype(jnp.bfloat16),
                values_new,
            )
        )
    for dialog in range(dialogs):
        parts = []
        for piece in range(1):
            part, part_new, values_new = weights[dialog * 1 + piece]
            summed = lax.dot_general(
                part, values[dialog], nn, preferred_element_type=jnp.float32
            ) + lax.dot_general(part_new, values_new, nn, preferred_element_type=jnp.float32)
            parts.append(summed[:, :HD] / summed[:, HD:])
        attended = jnp.concatenate(parts, axis=0)
        for head in range(heads):
            for index in range(fresh // block):
                first = head * fresh + index * block
                blocks[dialog * (fresh // block) + index, :, head * HD : (head + 1) * HD] = (
                    attended[first : first + block, :]
                )
    row, core = lax.axis_index("row"), lax.axis_index("core")
    order = [lax.rem(row + step, tensor_rows) for step in range(tensor_rows)]
    half = rows // 2
    mixed = jnp.concatenate(
        [blocks[2 * there + 1 - core] for there in order]
        + [blocks[2 * there + core] for there in order],
        axis=0,
    ).astype(jnp.bfloat16)
    for index in range(PANELS):
        span = slice(index * width, (index + 1) * width)
        product = lax.dot_general(
            mixed, weight[:, span], nn, preferred_element_type=jnp.float32
        ).astype(jnp.bfloat16)
        give[:, span] = product[:half]
        keep[:, span] = product[half:]


def attend(place, hist_len, queries, kv_new, pages, weight, tensor_rows):
    dialogs, entries = place.shape
    rows = queries.shape[0]
    out = jax.ShapeDtypeStruct((rows // 2, weight.shape[1]), jnp.bfloat16)
    smem = pl.BlockSpec(memory_space=pltpu.SMEM)
    vmem = pl.BlockSpec(memory_space=pltpu.VMEM)
    hbm = pl.BlockSpec(memory_space=pltpu.HBM)
    history = (dialogs, entries * PAGE, HD)
    return pl.pallas_call(
        functools.partial(attend_kernel, tensor_rows),
        out_shape=(out, out),
        in_specs=[smem, smem, vmem, vmem, vmem, vmem],
        out_specs=(vmem, vmem),
        scratch_shapes=[
            pltpu.VMEM((dialogs, entries) + pages.shape[1:], jnp.float32),
            pltpu.VMEM(kv_new.shape, jnp.float32),
            pltpu.VMEM(history, jnp.bfloat16),
            pltpu.VMEM(history[:2] + (2 * HD,), jnp.bfloat16),
            pltpu.VMEM((2 * tensor_rows, rows // (2 * tensor_rows), weight.shape[0]), jnp.float32),
        ],
        compiler_params=pltpu.CompilerParams(vmem_limit_bytes=24 * 1024 * 1024),
        name="attend",
    )(place, hist_len, queries, kv_new, pages, weight)


def sum_over_tensor(give, keep, tensor_rows):
    came = lax.ppermute(give, "core", [(0, 1), (1, 0)])
    block = give.shape[0] // tensor_rows
    wide = jnp.float32
    pair = [
        keep[step * block : (step + 1) * block].astype(wide)
        + came[step * block : (step + 1) * block].astype(wide)
        for step in range(tensor_rows)
    ]
    total = pair[0]
    for step in SENDING:
        turn = [(row, (row + step) % tensor_rows) for row in range(tensor_rows)]
        total = total + lax.ppermute(pair[step].astype(give.dtype), "row", turn).astype(wide)
    return total.astype(give.dtype)


def local(queries, kv_new, pool, page_table, hist_len, o_weight):
    groups = lax.axis_size(REPLICA)
    tensor_rows = lax.axis_size("row")
    shelves = pool.reshape(pool.shape[0], 2 * PAGE, HD)
    wanted, place = plan(page_table, hist_len, groups, pool.shape[0])
    asked = lax.all_to_all(wanted, REPLICA, split_axis=0, concat_axis=0, tiled=True)
    sent = collect(asked, shelves, groups)
    pages = lax.all_to_all(sent, REPLICA, split_axis=0, concat_axis=0, tiled=True)
    pages = pages.reshape(groups * SLOT, 2 * PAGE, HD)
    fresh = kv_new.reshape(2 * kv_new.shape[0], HD)
    give, keep = attend(place, hist_len, queries, fresh, pages, o_weight, tensor_rows)
    return sum_over_tensor(give, keep, tensor_rows)


def solution(mesh):
    split = Mesh(
        mesh.devices.reshape(4, 4, mesh.shape["tensor"] // 2, 2), REPLICA + TENSOR
    )
    in_specs = (
        P(REPLICA, TENSOR),
        P(REPLICA, None, TENSOR),
        P(REPLICA, None, None, TENSOR),
        P(REPLICA, None),
        P(REPLICA),
        P(TENSOR, None),
    )
    out_specs = P(REPLICA + TENSOR, None)
    return jax.shard_map(local, mesh=split, in_specs=in_specs, out_specs=out_specs, check_vma=False)
```

```python
import functools
import math

import jax
import jax.numpy as jnp
from jax import lax
from jax.experimental import pallas as pl
from jax.experimental.pallas import tpu as pltpu
from jax.sharding import Mesh
from jax.sharding import PartitionSpec as P

HD = 128
PAGE = 128
SLOT = 3
LANES = 128
PANELS = 8
SENDING = (1, 3, 2)
FLOOR = -1e30
SURE = 768
REPLICA = ("replica_0", "replica_1")
TENSOR = ("row", "core")


def plan_kernel(groups, pool_size, table, length, wanted, place, count):
    dialogs, entries = table.shape
    for owner in range(groups):
        count[owner] = 0
        for slot in range(SLOT):
            wanted[owner, 0, slot] = 0
    for dialog in range(dialogs):
        tokens = length[dialog]
        for entry in range(entries):
            page = table[dialog, entry]
            owner = lax.div(page, pool_size)
            live = entry * PAGE < tokens
            rank = count[owner]

            @pl.when(live)
            def _():
                wanted[owner, 0, rank] = page - owner * pool_size
                count[owner] = rank + 1

            place[dialog, entry] = jnp.where(live, owner * SLOT + rank, 0)


def plan(page_table, hist_len, groups, pool_size):
    smem = pl.BlockSpec(memory_space=pltpu.SMEM)
    return pl.pallas_call(
        functools.partial(plan_kernel, groups, pool_size),
        out_shape=(
            jax.ShapeDtypeStruct((groups, 1, LANES), jnp.int32),
            jax.ShapeDtypeStruct(page_table.shape, jnp.int32),
        ),
        in_specs=[smem, smem],
        out_specs=(smem, smem),
        scratch_shapes=[pltpu.SMEM((groups,), jnp.int32)],
        compiler_params=pltpu.CompilerParams(vmem_limit_bytes=60000 * 1024),
        cost_estimate=pl.CostEstimate(flops=10**10, bytes_accessed=10**7, transcendentals=0),
        name="plan",
    )(page_table, hist_len)


def collect_kernel(groups, asked, pool, out, ids, ids_sem):
    read = pltpu.make_async_copy(asked, ids, ids_sem)
    read.start()
    read.wait()
    for owner in range(groups):
        for slot in range(SLOT):
            out[owner, slot] = pool[ids[owner, 0, slot]]


def collect(asked, pool, groups):
    shape = (groups, SLOT) + pool.shape[1:]
    vmem = pl.BlockSpec(memory_space=pltpu.VMEM)
    return pl.pallas_call(
        functools.partial(collect_kernel, groups),
        out_shape=jax.ShapeDtypeStruct(shape, pool.dtype),
        in_specs=[pl.BlockSpec(memory_space=pl.ANY), vmem],
        out_specs=vmem,
        scratch_shapes=[pltpu.SMEM(asked.shape, jnp.int32), pltpu.SemaphoreType.DMA],
        compiler_params=pltpu.CompilerParams(vmem_limit_bytes=8 * 1024 * 1024),
        cost_estimate=pl.CostEstimate(flops=100000000000, bytes_accessed=100000000, transcendentals=0),
        name="collect",
    )(asked, pool)


def attend_kernel(
    tensor_rows,
    place,
    length,
    queries,
    kv_new,
    pages,
    weight,
    give,
    keep,
    wide,
    wide_new,
    keys,
    values,
    blocks,
):
    dialogs, entries = place.shape
    rows = queries.shape[0]
    fresh = rows // dialogs
    heads = queries.shape[1] // HD
    block = rows // (2 * tensor_rows)
    width = weight.shape[1] // PANELS
    rate = math.log2(math.e) / math.sqrt(HD)
    nt = (((1,), (1,)), ((), ()))
    nn = (((1,), (0,)), ((), ()))
    wide_new[...] = kv_new[...].astype(jnp.float32)
    for dialog in range(dialogs):
        values[dialog, :, HD:] = jnp.ones((entries * PAGE, HD), jnp.bfloat16)
        for entry in range(entries):
            wide[dialog, entry] = pages[place[dialog, entry]].astype(jnp.float32)
            span = slice(entry * PAGE, (entry + 1) * PAGE)
            keys[dialog, span, :] = wide[dialog, entry, pl.ds(0, PAGE, stride=2), :].astype(
                jnp.bfloat16
            )
            values[dialog, span, :HD] = wide[dialog, entry, pl.ds(1, PAGE, stride=2), :].astype(
                jnp.bfloat16
            )
    stage = []
    for dialog in range(dialogs):
        own = slice(dialog * fresh, (dialog + 1) * fresh)
        asked = jnp.concatenate(
            [queries[own, head * HD : (head + 1) * HD] for head in range(heads)], axis=0
        )
        start = dialog * 2 * fresh
        keys_new = wide_new[pl.ds(start, fresh, stride=2), :].astype(jnp.bfloat16)
        values_new = wide_new[pl.ds(start + 1, fresh, stride=2), :].astype(jnp.bfloat16)
        values_new = jnp.concatenate([values_new, jnp.ones_like(values_new)], axis=1)
        span = asked.shape[0] // 1
        for piece in range(1):
            some = asked[piece * span : (piece + 1) * span]
            score_new = lax.dot_general(some, keys_new, nt, preferred_element_type=jnp.float32)
            row = lax.broadcasted_iota(jnp.int32, score_new.shape, 0) % fresh
            col = lax.broadcasted_iota(jnp.int32, score_new.shape, 1)
            score_new = jnp.where(col <= row, score_new, FLOOR)
            score = lax.dot_general(some, keys[dialog], nt, preferred_element_type=jnp.float32)
            later = score[:, SURE:]
            token = SURE + lax.broadcasted_iota(jnp.int32, later.shape, 1)
            later = jnp.where(token < length[dialog], later, FLOOR)
            score = jnp.concatenate([score[:, :SURE], later], axis=1)
            stage.append((score, score_new, values_new))
    weights = []
    for score, score_new, values_new in stage:
        peak = jnp.maximum(
            jnp.max(score, axis=1, keepdims=True), jnp.max(score_new, axis=1, keepdims=True)
        )
        weights.append(
            (
                jnp.exp2((score - peak) * rate).astype(jnp.bfloat16),
                jnp.exp2((score_new - peak) * rate).astype(jnp.bfloat16),
                values_new,
            )
        )
    for dialog in range(dialogs):
        parts = []
        for piece in range(1):
            part, part_new, values_new = weights[dialog * 1 + piece]
            summed = lax.dot_general(
                part, values[dialog], nn, preferred_element_type=jnp.float32
            ) + lax.dot_general(part_new, values_new, nn, preferred_element_type=jnp.float32)
            parts.append(summed[:, :HD] / summed[:, HD:])
        attended = jnp.concatenate(parts, axis=0)
        for head in range(heads):
            for index in range(fresh // block):
                first = head * fresh + index * block
                blocks[dialog * (fresh // block) + index, :, head * HD : (head + 1) * HD] = (
                    attended[first : first + block, :]
                )
    row, core = lax.axis_index("row"), lax.axis_index("core")
    order = [lax.rem(row + step, tensor_rows) for step in range(tensor_rows)]
    half = rows // 2
    mixed = jnp.concatenate(
        [blocks[2 * there + 1 - core] for there in order]
        + [blocks[2 * there + core] for there in order],
        axis=0,
    ).astype(jnp.bfloat16)
    for index in range(PANELS):
        span = slice(index * width, (index + 1) * width)
        product = lax.dot_general(
            mixed, weight[:, span], nn, preferred_element_type=jnp.float32
        ).astype(jnp.bfloat16)
        give[:, span] = product[:half]
        keep[:, span] = product[half:]


def attend(place, hist_len, queries, kv_new, pages, weight, tensor_rows):
    dialogs, entries = place.shape
    rows = queries.shape[0]
    out = jax.ShapeDtypeStruct((rows // 2, weight.shape[1]), jnp.bfloat16)
    smem = pl.BlockSpec(memory_space=pltpu.SMEM)
    vmem = pl.BlockSpec(memory_space=pltpu.VMEM)
    hbm = pl.BlockSpec(memory_space=pltpu.HBM)
    history = (dialogs, entries * PAGE, HD)
    return pl.pallas_call(
        functools.partial(attend_kernel, tensor_rows),
        out_shape=(out, out),
        in_specs=[smem, smem, vmem, vmem, vmem, vmem],
        out_specs=(vmem, vmem),
        scratch_shapes=[
            pltpu.VMEM((dialogs, entries) + pages.shape[1:], jnp.float32),
            pltpu.VMEM(kv_new.shape, jnp.float32),
            pltpu.VMEM(history, jnp.bfloat16),
            pltpu.VMEM(history[:2] + (2 * HD,), jnp.bfloat16),
            pltpu.VMEM((2 * tensor_rows, rows // (2 * tensor_rows), weight.shape[0]), jnp.float32),
        ],
        compiler_params=pltpu.CompilerParams(vmem_limit_bytes=24 * 1024 * 1024),
        name="attend",
    )(place, hist_len, queries, kv_new, pages, weight)


def sum_over_tensor(give, keep, tensor_rows):
    came = lax.ppermute(give, "core", [(0, 1), (1, 0)])
    block = give.shape[0] // tensor_rows
    wide = jnp.float32
    pair = [
        keep[step * block : (step + 1) * block].astype(wide)
        + came[step * block : (step + 1) * block].astype(wide)
        for step in range(tensor_rows)
    ]
    total = pair[0]
    sent = lax.optimization_barrier(tuple(pair[step].astype(give.dtype) for step in SENDING))
    for step, block in zip(SENDING, sent):
        turn = [(row, (row + step) % tensor_rows) for row in range(tensor_rows)]
        total = total + lax.ppermute(block, "row", turn).astype(wide)
    return total.astype(give.dtype)


def local(queries, kv_new, pool, page_table, hist_len, o_weight):
    groups = lax.axis_size(REPLICA)
    tensor_rows = lax.axis_size("row")
    shelves = pool.reshape(pool.shape[0], 2 * PAGE, HD)
    wanted, place = plan(page_table, hist_len, groups, pool.shape[0])
    asked = lax.all_to_all(wanted, REPLICA, split_axis=0, concat_axis=0, tiled=True)
    sent = collect(asked, shelves, groups)
    pages = lax.all_to_all(sent, REPLICA, split_axis=0, concat_axis=0, tiled=True)
    pages = pages.reshape(groups * SLOT, 2 * PAGE, HD)
    fresh = kv_new.reshape(2 * kv_new.shape[0], HD)
    give, keep = attend(place, hist_len, queries, fresh, pages, o_weight, tensor_rows)
    return sum_over_tensor(give, keep, tensor_rows)


def solution(mesh):
    split = Mesh(
        mesh.devices.reshape(4, 4, mesh.shape["tensor"] // 2, 2), REPLICA + TENSOR
    )
    in_specs = (
        P(REPLICA, TENSOR),
        P(REPLICA, None, TENSOR),
        P(REPLICA, None, None, TENSOR),
        P(REPLICA, None),
        P(REPLICA),
        P(TENSOR, None),
    )
    out_specs = P(REPLICA + TENSOR, None)
    return jax.shard_map(local, mesh=split, in_specs=in_specs, out_specs=out_specs, check_vma=False)
```
